128 devices in a mesh: wide: 32 (over y, z, core), narrow: 4 (over x).
Axes of the slice: x: 4, y: 4, z: 4, core: 2. Of those that a mesh axis runs over, the one named last changes fastest.
Arguments:
- object_field: float32 [2, 2048, 16384], P(None, 'narrow', 'wide')
- probe: float32 [4, 2, 256, 256], replicated, may hold values from -3 to 3
- patterns: float32 [4, 32, 6, 256, 256], P('narrow', 'wide'), may hold values from 0.1 to 4
- offsets: int32 [4, 32, 6, 2], P('narrow', 'wide'), may hold values from -128 to 384
- counts: int32 [4, 32], P('narrow', 'wide'), may hold values from 1 to 6
Outputs:
- object_new: float32 [2, 2048, 16384], P(None, 'narrow', 'wide')
- probe_new: float32 [4, 2, 256, 256], replicated
The draws below stay inside these ranges and needn't reach their ends.
Inputs may be any that keep to these rules, and one draw needn't show every extreme that they name: A patch of 256 x 256 pixels at these offsets stays within the tile extended by 128 pixels on each side. `counts`: slots 0 to count - 1 of a tile are live, the others are ignored.
All inputs are finite; a program needn't handle non-finite values.
Results may differ from the reference program's by a relative error of at most 0.0003.
Values sent between devices are 32-bit elements; how exact they have to be, the bound alone decides.
A program may use at most 128 MiB of HBM per device.

```python
import math
import jax
import jax.numpy as jnp
from jax import lax

R = 256
MODES = 4
TILE = 512
H = 128
BATCHES = 3
POS = 2
SLOTS = 6
NX = 2048
NY = 16384
N_WIDE = 32
N_NARROW = 4


def draw_object_field(key, part):
    columns = jnp.arange(NY, dtype=jnp.float32)
    ramp = 0.5 * (1.0 + 2.0 * columns / NY)
    values = jax.random.normal(key, (2, NX, NY), jnp.float32)
    return values * ramp[None, None, :]


def with_ends(entries, stream_key, smallest, high):
    extent = entries.shape
    index_at = [jax.random.randint(jax.random.fold_in(stream_key, axis), (), 0, extent[axis]) for axis in range(len(extent))]
    entries = entries.at[tuple(index_at)].set(smallest)
    longest = extent.index(max(extent))
    index_at[longest] = (index_at[longest] + 1) % extent[longest]
    return entries.at[tuple(index_at)].set(high)


def shard_levels(key, shape, pieces, smallest, high):
    gain, own = 1.0, jax.random.fold_in(key, 6)
    for dim, parts in pieces:
        draws = jnp.exp(jax.random.uniform(jax.random.fold_in(own, dim), (parts,), jnp.float32, smallest / len(pieces), high / len(pieces)))
        gain = gain * jnp.repeat(draws, shape[dim] // parts).reshape([-1 if axis == dim else 1 for axis in range(len(shape))])
    return gain


def bell_draw(stream_key, dims, width, reach, kind=jnp.bfloat16):
    array = width * jax.random.normal(stream_key, dims, jnp.float32)
    return jnp.clip(array, min=-reach, max=reach).astype(kind)


def setup_inputs(seed: int = 0) -> dict:
    seeds = jax.random.split(jax.random.key(seed), 6)
    object_field = draw_object_field(jax.random.fold_in(seeds[5], 71), 0)
    probe = bell_draw(seeds[1], (MODES, 2, R, R), 0.5, 3.0, jnp.float32)
    patterns = jnp.clip(jnp.exp(math.log(4.0) - 3.6888794 * jax.random.uniform(seeds[2], (N_NARROW, N_WIDE, SLOTS, R, R), jnp.float32) ** shard_levels(seeds[2], (N_NARROW, N_WIDE, SLOTS, R, R), ((0, 4), (1, 32)), -0.2, 0.2)), 0.1, 4.0)
    offsets = with_ends(jax.random.randint(seeds[3], (N_NARROW, N_WIDE, SLOTS, 2), 0 - H, TILE + H - R + 1), jax.random.fold_in(seeds[3], 1), 0 - H, TILE + H - R).astype(jnp.int32)
    counts = with_ends(jax.random.randint(seeds[4], (N_NARROW, N_WIDE), 1, SLOTS + 1), jax.random.fold_in(seeds[4], 1), 1, SLOTS).astype(jnp.int32)
    return dict(object_field=object_field, probe=probe, patterns=patterns, offsets=offsets, counts=counts)


def slot_terms(patch, probe, measured):
    probe_re = probe[:, 0]
    probe_im = probe[:, 1]
    obj_re = patch[0]
    obj_im = patch[1]
    psi = probe_re * obj_re - probe_im * obj_im + 1j * (probe_re * obj_im + probe_im * obj_re)
    far = jnp.fft.fft2(psi, norm='ortho')
    intensity = lax.optimization_barrier(jnp.sum(jnp.real(far) ** 2 + jnp.imag(far) ** 2, axis=0))
    ratio = jnp.sqrt(measured) / jnp.sqrt(intensity + 0.1)
    back = jnp.fft.ifft2(far * (1.0 - ratio), norm='ortho')
    back_re = jnp.real(back)
    back_im = jnp.imag(back)
    grad_re = lax.optimization_barrier(jnp.sum(probe_re * back_re + probe_im * back_im, axis=0))
    grad_im = lax.optimization_barrier(jnp.sum(probe_re * back_im - probe_im * back_re, axis=0))
    pgrad_re = obj_re * back_re + obj_im * back_im
    pgrad_im = obj_re * back_im - obj_im * back_re
    square = jnp.sum(obj_re * obj_re + obj_im * obj_im)
    return (jnp.stack([grad_re, grad_im]), jnp.stack([pgrad_re, pgrad_im], axis=1), square)

def reference(object_field, probe, patterns, offsets, counts):
    padded = jnp.pad(object_field, ((0, 0), (H, H), (H, H)))
    gradient = jnp.zeros_like(padded)
    flat_patterns = patterns.reshape(N_NARROW * N_WIDE, SLOTS, R, R)
    flat_offsets = offsets.reshape(N_NARROW * N_WIDE, SLOTS, 2)
    flat_counts = counts.reshape(N_NARROW * N_WIDE)
    devices_at = jnp.arange(N_NARROW * N_WIDE, dtype=jnp.int32)
    for minibatch in range(BATCHES):

        def visit(carry, inputs):
            gradient, probe_grad, coverage = carry
            measured_all, offs_all, count_here, device = inputs
            tile_row = device // N_WIDE * TILE
            tile_col = device % N_WIDE * TILE
            for position in range(POS):
                slot_at = minibatch * POS + position
                live = (slot_at < count_here).astype(jnp.float32)
                row_at = (tile_row + offs_all[slot_at, 0] + H).astype(jnp.int32)
                col_at = (tile_col + offs_all[slot_at, 1] + H).astype(jnp.int32)
                zero_at = jnp.zeros((), jnp.int32)
                patch = lax.dynamic_slice(padded, (zero_at, row_at, col_at), (2, R, R))
                obj_grad, pgrad, square = slot_terms(patch, probe, measured_all[slot_at])
                old = lax.dynamic_slice(gradient, (zero_at, row_at, col_at), (2, R, R))
                gradient = lax.dynamic_update_slice(gradient, old + live * obj_grad, (zero_at, row_at, col_at))
                probe_grad = probe_grad + live * pgrad
                coverage = coverage + live * square
            return ((gradient, probe_grad, coverage), None)
        start = (gradient, jnp.zeros_like(probe), jnp.zeros((), jnp.float32))
        (gradient, probe_grad, coverage), _ = lax.scan(visit, start, (flat_patterns, flat_offsets, flat_counts, devices_at))
        probe = probe - probe_grad / (coverage / (R * R))
    power = lax.optimization_barrier(jnp.sum(probe[:, 0] ** 2 + probe[:, 1] ** 2, axis=0))
    top = jnp.max(power)
    core = gradient[:, H:H + NX, H:H + NY]
    return (object_field - 0.5 * core / top, probe)
```

```python
import jax
import jax.numpy as jnp
import ml_dtypes
import numpy as np
from jax import lax
from jax.experimental import pallas as pl
from jax.experimental.pallas import tpu as pltpu
from jax.sharding import PartitionSpec as P

H = 128
TILE = 512
R = 256
HALF = R // 2
MODES = 4
BATCHES = 3
POS = 2
MESH = pl.DeviceIdType.MESH
F32 = jnp.float32
BF16 = jnp.bfloat16

PARTS = 3
CHUNKS = 16
ROWS = 24
ORDER = ((0, 1, 2), (1, 2, 0), (2, 0, 1))
STEPS = (1, 2, 3)


def tables():
    k = np.arange(R)
    angle = 2.0 * np.pi * ((np.arange(HALF)[:, None] * k[None, :]) % R) / R
    upper = np.cos(angle)
    lower = np.sin(angle)
    lower[0] = np.where(k % 2 == 0, 1.0, -1.0)
    packed = (np.concatenate([upper, lower]) / np.sqrt(R)).astype(np.float32)
    order = np.concatenate([np.arange(HALF), [HALF], R - np.arange(1, HALF)])
    select = np.zeros((R, R), np.float32)
    select[np.arange(R), order] = 1.0

    def pair(value):
        high = value.astype(ml_dtypes.bfloat16)
        low = (value - high.astype(np.float32)).astype(ml_dtypes.bfloat16)
        return [high, low]

    pick = select.astype(ml_dtypes.bfloat16)
    return np.stack(pair(packed) + pair(packed.T.copy()) + [pick, pick.T.copy()])


def split(value):
    high = value.astype(BF16)
    return high, (value - high.astype(F32)).astype(BF16)


def dot(a, b):
    return jnp.dot(a, b, preferred_element_type=F32)


def left_product(table, value):
    high, low = split(value)
    return dot(table[0], high) + dot(table[0], low) + dot(table[1], high)


def right_product(value, table):
    high, low = split(value)
    return dot(high, table[0]) + dot(low, table[0]) + dot(high, table[1])


def row_mask(shape):
    return lax.broadcasted_iota(jnp.int32, shape, 0) == 0


def rows_fixed(first, general):
    top = jnp.where(row_mask(first[:8].shape), first[:8], general[:8])
    return jnp.concatenate([top, general[8:]], axis=0)


def butterfly(zr, zi):
    ur, vr, ui, vi = zr[:HALF], zr[HALF:], zi[:HALF], zi[HALF:]
    plus = (rows_fixed(ur, ur + vi), rows_fixed(ui, ui - vr))
    minus = (rows_fixed(vr, ur - vi), rows_fixed(vi, ui + vr))
    first = lax.broadcasted_iota(jnp.int32, (HALF, HALF), 1) == 0
    out = []
    for re, im in (plus, minus):
        ur, vr, ui, vi = re[:, :HALF], re[:, HALF:], im[:, :HALF], im[:, HALF:]
        mr, mi = jnp.where(first, 0.0, vr), jnp.where(first, 0.0, vi)
        out.append(
            (
                (ur + mi, ui - mr),
                (jnp.where(first, vr, ur - vi), jnp.where(first, vi, ui + vr)),
            )
        )
    return out


def butterfly_transposed(quads):
    first = lax.broadcasted_iota(jnp.int32, (HALF, HALF), 1) == 0
    sides = []
    for (pr, pi), (qr, qi) in quads:
        ur = pr + jnp.where(first, 0.0, qr)
        ui = pi + jnp.where(first, 0.0, qi)
        vr = jnp.where(first, qr, qi - pi)
        vi = jnp.where(first, qi, pr - qr)
        sides.append((jnp.concatenate([ur, vr], axis=1), jnp.concatenate([ui, vi], axis=1)))
    (pr, pi), (qr, qi) = sides
    ur = rows_fixed(pr, pr + qr)
    ui = rows_fixed(pi, pi + qi)
    vr = rows_fixed(qr, qi - pi)
    vi = rows_fixed(qi, pr - qr)
    return jnp.concatenate([ur, vr, ui, vi], axis=0)


def read_plane(ref, plane):
    if plane == 3:
        value = ref[pl.ds(2 * CHUNKS, CHUNKS), pl.ds(0, 16), :]
        return value.reshape(R, R)
    start, stop = plane * R, (plane + 1) * R
    low, high = start // ROWS, -(-stop // ROWS)
    value = ref[pl.ds(low, high - low)].reshape((high - low) * ROWS, R)
    return value[start - low * ROWS : stop - low * ROWS]


def write_plane(ref, plane, value):
    if plane == 3:
        for chunk in range(CHUNKS):
            ref[2 * CHUNKS + chunk, pl.ds(0, 16), :] = value[16 * chunk : 16 * chunk + 16]
        return
    for tile in range(R // 8):
        row = plane * R + 8 * tile
        ref[row // ROWS, pl.ds(row % ROWS, 8), :] = value[8 * tile : 8 * tile + 8]


def whole_kernel(
    offs, cnt, obj, probe, patterns, tabs,
    obj_out, probe_out,
    pad, pbuf, gbuf, spat, patch, far, og, zbuf, grad, cover,
    acc0, acc1, recv0, recv1, recv2, cross, hside, hvert, hcorn,
    bsend, brecv, hsend, hrecv, gsend, grecv,
):
    wide = lax.axis_index("wide")
    x = lax.axis_index("narrow")
    n_wide = lax.axis_size("wide")
    n_narrow = lax.axis_size("narrow")
    core = wide % 2
    z = (wide // 2) % 4
    y = wide // 8
    place = (x, y, z)
    table = (tabs.at[0], tabs.at[1])
    table_t = (tabs.at[2], tabs.at[3])

    def device(at, c):
        return ((at[1] * 4 + at[2]) * 2 + c, at[0])

    def peer(dim, step):
        at = list(place)
        at[dim] = (at[dim] + step) % 4
        return device(at, core)

    sibling = device(place, 1 - core)

    ways = ((-1, 0), (1, 0), (0, -1), (0, 1), (-1, -1), (1, -1), (-1, 1), (1, 1))

    def there(way):
        dw, dn = way
        ok = wide >= 0
        if dw:
            ok = (wide > 0) if dw < 0 else (wide < n_wide - 1)
        if dn:
            ok_n = (x > 0) if dn < 0 else (x < n_narrow - 1)
            ok = jnp.logical_and(ok, ok_n) if dw else ok_n
        return ok

    def away(way):
        return (wide + way[0], x + way[1])

    def border(way):
        dw, dn = way
        lane = {-1: (0, 1), 0: (1, 4), 1: (5, 1)}[dw]
        row = {-1: (0, H), 0: (H, TILE), 1: (H + TILE, H)}[dn]
        return lane, row

    def edge(way):
        dw, dn = way
        lane = {-1: (0, 1), 0: (0, 4), 1: (3, 1)}[dw]
        row = {-1: (0, H), 0: (0, TILE), 1: (TILE - H, H)}[dn]
        return lane, row

    for at in range(2):
        for lane in (0, 5):
            pad[at, lane] = jnp.zeros((TILE + 2 * H, H), F32)
        for lane in range(1, 5):
            pad[at, lane, pl.ds(0, H), :] = jnp.zeros((H, H), F32)
            pad[at, lane, pl.ds(H + TILE, H), :] = jnp.zeros((H, H), F32)
    hside[...] = jnp.zeros_like(hside)
    hvert[...] = jnp.zeros_like(hvert)
    hcorn[...] = jnp.zeros_like(hcorn)

    barrier = pltpu.get_barrier_semaphore()
    pl.semaphore_signal(barrier, inc=1, device_id=sibling, device_id_type=MESH)
    for dim in range(3):
        for step in STEPS:
            pl.semaphore_signal(barrier, inc=1, device_id=peer(dim, step), device_id_type=MESH)
    total = 10
    for way in ways:
        total = total + there(way).astype(jnp.int32)

        @pl.when(there(way))
        def _():
            pl.semaphore_signal(barrier, inc=1, device_id=away(way), device_id_type=MESH)

    pl.semaphore_wait(barrier, total)

    def halo(way, slot, lane):
        (lane_to, _), (row_to, rows) = border((-way[0], -way[1]))
        (lane_from, _), (row_from, _) = edge(way)
        return pltpu.make_async_remote_copy(
            src_ref=obj.at[:, pl.ds(row_from, rows), pl.ds((lane_from + lane) * H, H)],
            dst_ref=pad.at[:, lane_to + lane, pl.ds(row_to, rows), :],
            send_sem=hsend.at[slot],
            recv_sem=hrecv.at[slot],
            device_id=away(way),
            device_id_type=MESH,
        )

    halos = []
    for way in (2, 3, 4, 5, 6, 7, 0, 1):
        for lane in range(4 if ways[way][0] == 0 else 1):
            halos.append((ways[way], len(halos), lane))
    for way, slot, lane in halos:

        @pl.when(there(way))
        def _():
            halo(way, slot, lane).start()

    for at in range(2):
        for lane in range(4):
            pad[at, lane + 1, pl.ds(H, TILE), :] = obj[at, :, pl.ds(lane * H, H)]
    for half in range(2):
        for plane in range(4):
            write_plane(pbuf.at[0, half], plane, probe[half * 2 + plane // 2, plane % 2])
        for chunk in range(CHUNKS):
            pbuf[0, half, 2 * CHUNKS + chunk, pl.ds(16, 8), :] = jnp.zeros((8, R), F32)
    zbuf[...] = jnp.zeros_like(zbuf)
    grad[...] = jnp.zeros_like(grad)

    @pl.loop(0, BATCHES * POS)
    def _(slot):
        high, low = split(jnp.sqrt(patterns[slot]))
        high, low = split(dot(tabs[4], high) + dot(tabs[4], low))
        spat[slot] = dot(high, tabs[5]) + dot(low, tabs[5])

    for way, slot, lane in halos:

        @pl.when(there(way))
        def _():
            halo(way, slot, lane).wait_send()

        @pl.when(there((-way[0], -way[1])))
        def _():
            halo(way, slot, lane).wait_recv()

    lanes = lax.broadcasted_iota(jnp.int32, (R, H), 1)

    def window(slot):
        row = offs[2 * slot] + H
        col = offs[2 * slot + 1] + H
        first = jnp.minimum(col // H, 3)
        return row, first, col - first * H

    def take_patches(batch):
        covered = jnp.zeros((8, R), F32)
        for position in range(POS):
            slot = batch * POS + position
            row, first, shift = window(slot)
            live = slot < cnt[0]
            turn = (H - shift) % H
            for at in range(2):
                turned = [
                    pltpu.roll(pad[at, first + k, pl.ds(row, R), :], turn, 1) for k in range(3)
                ]
                for k in range(2):
                    value = jnp.where(lanes < H - shift, turned[k], turned[k + 1])
                    value = jnp.where(live, value, 0.0)
                    patch[position, at, :, pl.ds(k * H, H)] = value
                    covered = covered + jnp.sum(value * value)
        cover[...] = covered

    take_patches(0)

    def half_planes(ref, mode):
        return read_plane(ref, 2 * mode), read_plane(ref, 2 * mode + 1)

    def run_batch(batch):
        for half in range(2):
            for chunk in range(CHUNKS):
                gbuf[half, 2 * CHUNKS + chunk, pl.ds(16, 8), :] = cover[...]

        @pl.loop(0, 2)
        def _(half):
            for mode in range(2):
                pr, pi = half_planes(pbuf.at[batch, half], mode)
                for position in range(POS):
                    our, oui = patch[position, 0], patch[position, 1]
                    psi = jnp.concatenate([pr * our - pi * oui, pr * oui + pi * our], axis=1)
                    left = left_product((table[0][...], table[1][...]), psi)
                    left = jnp.concatenate([left[:, :R], left[:, R:]], axis=0)
                    both = right_product(left, (table_t[0][...], table_t[1][...]))
                    quads = butterfly(both[:R], both[R:])
                    slot = half * 2 + mode
                    for a in range(2):
                        for b in range(2):
                            for at in range(2):
                                far[position, slot, at, pl.ds(a * HALF, HALF), pl.ds(b * HALF, HALF)] = (
                                    quads[a][b][at]
                                )

        for position in range(POS):

            @pl.loop(0, R // 32)
            def _(tile):
                rows = pl.ds(pl.multiple_of(tile * 32, 32), 32)
                power = jnp.zeros((32, R), F32)
                for mode in range(MODES):
                    re, im = far[position, mode, 0, rows, :], far[position, mode, 1, rows, :]
                    power = power + re * re + im * im
                slot = batch * POS + position
                spat[slot, rows, :] = 1.0 - spat[slot, rows, :] * lax.rsqrt(power + 0.1)

        @pl.loop(0, 2)
        def _(half):
            for mode in range(2):
                pr, pi = half_planes(pbuf.at[batch, half], mode)
                sum_re, sum_im = None, None
                for position in range(POS):
                    slot = half * 2 + mode
                    quads = []
                    for a in range(2):
                        row = []
                        for b in range(2):
                            rows, cols = pl.ds(a * HALF, HALF), pl.ds(b * HALF, HALF)
                            keep = spat[batch * POS + position, rows, cols]
                            row.append(
                                (
                                    far[position, slot, 0, rows, cols] * keep,
                                    far[position, slot, 1, rows, cols] * keep,
                                )
                            )
                        quads.append(row)
                    both = butterfly_transposed(quads)
                    right = right_product(both, (table[0][...], table[1][...]))
                    right = jnp.concatenate([right[:R], right[R:]], axis=1)
                    back = left_product((table_t[0][...], table_t[1][...]), right)
                    dr, di = back[:, :R], back[:, R:]
                    our, oui = patch[position, 0], patch[position, 1]
                    og_re = pr * dr + pi * di
                    og_im = pr * di - pi * dr
                    if mode == 0:

                        @pl.when(half == 0)
                        def _():
                            og[position, 0] = og_re
                            og[position, 1] = og_im

                        @pl.when(half != 0)
                        def _():
                            og[position, 0] += og_re
                            og[position, 1] += og_im
                    else:
                        og[position, 0] += og_re
                        og[position, 1] += og_im
                    pg_re = our * dr + oui * di
                    pg_im = our * di - oui * dr
                    sum_re = pg_re if sum_re is None else sum_re + pg_re
                    sum_im = pg_im if sum_im is None else sum_im + pg_im
                write_plane(gbuf.at[half], 2 * mode, sum_re)
                write_plane(gbuf.at[half], 2 * mode + 1, sum_im)

    def add_gradient(batch):
        rows, firsts = [], []
        for position in range(POS):
            row, first, shift = window(batch * POS + position)
            rows.append(row)
            firsts.append(first)
            turn = shift % H
            for at in range(2):
                low = pltpu.roll(og[position, at, :, pl.ds(0, H)], turn, 1)
                high = pltpu.roll(og[position, at, :, pl.ds(H, H)], turn, 1)
                zbuf[position, at, 1, pl.ds(8, R), :] = jnp.where(lanes >= shift, low, 0.0)
                zbuf[position, at, 2, pl.ds(8, R), :] = jnp.where(lanes >= shift, high, low)
                zbuf[position, at, 3, pl.ds(8, R), :] = jnp.where(lanes >= shift, 0.0, high)

        @pl.loop(0, (TILE + 2 * H) // 16)
        def _(tile):
            base = pl.multiple_of(tile * 16, 16)
            for sub in range(2):
                at_row = base + 8 * sub
                starts = [jnp.clip(at_row - row + 8, 0, R + 8) for row in rows]
                for at in range(2):
                    for lane in range(6):
                        value = grad[at, lane, pl.ds(at_row, 8), :]
                        for position in range(POS):
                            source = jnp.clip(lane - firsts[position] + 1, 0, 4)
                            value = value + zbuf[position, at, source, pl.ds(starts[position], 8), :]
                        grad[at, lane, pl.ds(at_row, 8), :] = value

    def border_copy(index):
        way = ways[index]
        (lane, n_lane), (row, rows) = border(way)
        if way[1] == 0:
            source = grad.at[:, lane, pl.ds(row, rows), :]
            target = hside.at[index]
        elif way[0] == 0:
            source = grad.at[:, pl.ds(lane, n_lane), pl.ds(row, rows), :]
            target = hvert.at[index - 2]
        else:
            source = grad.at[:, lane, pl.ds(row, rows), :]
            target = hcorn.at[index - 4]
        return pltpu.make_async_remote_copy(
            src_ref=source,
            dst_ref=target,
            send_sem=gsend.at[index],
            recv_sem=grecv.at[index],
            device_id=away(way),
            device_id_type=MESH,
        )

    def all_reduce(batch):
        new = pbuf.at[batch + 1]
        old = pbuf.at[batch]

        def copy(source, target, index, to):
            return pltpu.make_async_remote_copy(
                src_ref=source,
                dst_ref=target,
                send_sem=bsend.at[index],
                recv_sem=brecv.at[batch, index],
                device_id=to,
                device_id_type=MESH,
            )

        sent = []

        def send(*args):
            one = copy(*args)
            one.start()
            sent.append(one)

        other = 1 - core
        for part in range(PARTS):
            span = pl.ds(part * CHUNKS, CHUNKS)
            send(gbuf.at[other, span], recv0.at[batch, span], part, sibling)
        for part in range(PARTS):
            span = pl.ds(part * CHUNKS, CHUNKS)
            d1 = ORDER[part][0]
            copy(gbuf.at[other, span], recv0.at[batch, span], part, sibling).wait_recv()
            acc0[span] = gbuf[core, span] + recv0[batch, span]
            for step in STEPS:
                index = 3 + part * 3 + step - 1
                chunk = part * CHUNKS + 4 * ((place[d1] + step) % 4)
                send(acc0.at[pl.ds(chunk, 4)], recv1.at[batch, part, step - 1], index, peer(d1, step))

        take_patches(jnp.minimum(batch + 1, BATCHES - 1))

        for part in range(PARTS):
            d1, d2, _ = ORDER[part]
            own = pl.ds(part * CHUNKS + 4 * place[d1], 4)
            value = acc0[own]
            for step in STEPS:
                index = 3 + part * 3 + step - 1
                copy(acc0.at[own], recv1.at[batch, part, step - 1], index, peer(d1, step)).wait_recv()
                value = value + recv1[batch, part, step - 1]
            acc1[part] = value
            for step in STEPS:
                index = 12 + part * 3 + step - 1
                send(acc1.at[part, (place[d2] + step) % 4], recv2.at[batch, part, step - 1], index, peer(d2, step))

        add_gradient(batch)

        @pl.when(batch == BATCHES - 1)
        def _():
            for index in (2, 3, 4, 5, 6, 7, 0, 1):

                @pl.when(there(ways[index]))
                def _():
                    border_copy(index).start()

        for part in range(PARTS):
            _, d2, d3 = ORDER[part]
            value = acc1[part, place[d2]]
            for step in STEPS:
                index = 12 + part * 3 + step - 1
                copy(acc1.at[part, 0], recv2.at[batch, part, step - 1], index, peer(d2, step)).wait_recv()
                value = value + recv2[batch, part, step - 1]
            cross[batch, part, place[d3]] = value
            for step in STEPS:
                index = 21 + part * 3 + step - 1
                mine = cross.at[batch, part, place[d3]]
                send(mine, mine, index, peer(d3, step))
        sums = []
        for part in range(PARTS):
            d3 = ORDER[part][2]
            for step in STEPS:
                index = 21 + part * 3 + step - 1
                theirs = cross.at[batch, part, (place[d3] + 4 - step) % 4]
                copy(theirs, theirs, index, peer(d3, step)).wait_recv()
            value = cross[batch, part, 0]
            for at in range(1, 4):
                value = value + cross[batch, part, at]
            sums.append(value)
        scale = sums[2][16:] / float(R * R)
        scale = jnp.concatenate([scale, scale, scale], axis=0)
        for part in range(PARTS):
            d1, d2, _ = ORDER[part]
            chunk = part * CHUNKS + 4 * place[d1] + place[d2]
            new[core, chunk] = old[core, chunk] - sums[part] / scale
            for step in STEPS:
                index = 30 + part * 3 + step - 1
                mine = new.at[core, chunk]
                send(mine, mine, index, peer(d2, step))
        for part in range(PARTS):
            d1, d2, _ = ORDER[part]
            for step in STEPS:
                index = 30 + part * 3 + step - 1
                chunk = part * CHUNKS + 4 * place[d1] + (place[d2] + 4 - step) % 4
                theirs = new.at[core, chunk]
                copy(theirs, theirs, index, peer(d2, step)).wait_recv()
            group = new.at[core, pl.ds(part * CHUNKS + 4 * place[d1], 4)]
            for step in STEPS:
                send(group, group, 39 + part * 3 + step - 1, peer(d1, step))
            send(group, group, 48 + part * 4, sibling)
        for step in STEPS:
            for part in range(PARTS):
                d1 = ORDER[part][0]
                group = new.at[core, pl.ds(part * CHUNKS + 4 * ((place[d1] + 4 - step) % 4), 4)]
                copy(group, group, 39 + part * 3 + step - 1, peer(d1, step)).wait_recv()
                send(group, group, 48 + part * 4 + step, sibling)
        for step in range(4):
            for part in range(PARTS):
                d1 = ORDER[part][0]
                group = new.at[other, pl.ds(part * CHUNKS + 4 * ((place[d1] + 4 - step) % 4), 4)]
                copy(group, group, 48 + part * 4 + step, sibling).wait_recv()
        for one in sent:
            one.wait_send()

    @pl.loop(0, BATCHES)
    def _(batch):
        run_batch(batch)
        all_reduce(batch)

    power = jnp.zeros((R, R), F32)
    for half in range(2):
        for plane in range(4):
            value = read_plane(pbuf.at[BATCHES, half], plane)
            probe_out[half * 2 + plane // 2, plane % 2] = value
            power = power + value * value
    top = jnp.max(power)

    for index, way in enumerate(ways):

        @pl.when(there(way))
        def _():
            border_copy(index).wait_send()

        @pl.when(there((-way[0], -way[1])))
        def _():
            border_copy(index).wait_recv()

    def came(lane, row, rows, at):
        value = grad[at, lane + 1, pl.ds(H + row, rows), :]
        if lane == 0:
            value = value + hside[1, at, pl.ds(row, rows), :]
        if lane == 3:
            value = value + hside[0, at, pl.ds(row, rows), :]
        if row == 0:
            value = value + hvert[1, at, lane]
            if lane == 0:
                value = value + hcorn[3, at]
            if lane == 3:
                value = value + hcorn[2, at]
        if row == TILE - H:
            value = value + hvert[0, at, lane]
            if lane == 0:
                value = value + hcorn[1, at]
            if lane == 3:
                value = value + hcorn[0, at]
        return value

    for at in range(2):
        for lane in range(4):
            for row in range(0, TILE, H):
                place_at = (at, pl.ds(row, H), pl.ds(lane * H, H))
                obj_out[place_at] = obj[place_at] - 0.5 * came(lane, row, H, at) / top


def local(object_field, probe, patterns, offsets, counts):
    vmem = pl.BlockSpec(memory_space=pltpu.VMEM)
    smem = pl.BlockSpec(memory_space=pltpu.SMEM)
    dma = pltpu.SemaphoreType.DMA
    return pl.pallas_call(
        whole_kernel,
        out_shape=(
            jax.ShapeDtypeStruct((2, TILE, TILE), F32),
            jax.ShapeDtypeStruct((MODES, 2, R, R), F32),
        ),
        in_specs=[smem, smem, vmem, vmem, vmem, vmem],
        out_specs=(vmem, vmem),
        scratch_shapes=[
            pltpu.VMEM((2, 6, TILE + 2 * H, H), F32),
            pltpu.VMEM((BATCHES + 1, 2, PARTS * CHUNKS, ROWS, R), F32),
            pltpu.VMEM((2, PARTS * CHUNKS, ROWS, R), F32),
            pltpu.VMEM((BATCHES * POS, R, R), F32),
            pltpu.VMEM((POS, 2, R, R), F32),
            pltpu.VMEM((POS, MODES, 2, R, R), F32),
            pltpu.VMEM((POS, 2, R, R), F32),
            pltpu.VMEM((POS, 2, 5, R + 16, H), F32),
            pltpu.VMEM((2, 6, TILE + 2 * H, H), F32),
            pltpu.VMEM((8, R), F32),
            pltpu.VMEM((PARTS * CHUNKS, ROWS, R), F32),
            pltpu.VMEM((PARTS, 4, ROWS, R), F32),
            pltpu.VMEM((BATCHES, PARTS * CHUNKS, ROWS, R), F32),
            pltpu.VMEM((BATCHES, PARTS, 3, 4, ROWS, R), F32),
            pltpu.VMEM((BATCHES, PARTS, 3, ROWS, R), F32),
            pltpu.VMEM((BATCHES, PARTS, 4, ROWS, R), F32),
            pltpu.VMEM((2, 2, TILE, H), F32),
            pltpu.VMEM((2, 2, 4, H, H), F32),
            pltpu.VMEM((4, 2, H, H), F32),
            dma((60,)),
            dma((BATCHES, 60)),
            dma((14,)),
            dma((14,)),
            dma((8,)),
            dma((8,)),
        ],
        compiler_params=pltpu.CompilerParams(
            collective_id=0, has_side_effects=True, vmem_limit_bytes=67043328
        ),
    )(
        offsets.reshape(BATCHES * POS * 2),
        counts.reshape(1),
        object_field,
        probe,
        patterns.reshape(BATCHES * POS, R, R),
        jnp.asarray(tables()),
    )


def solution(mesh):
    placed = (
        P(None, "narrow", "wide"),
        P(),
        P("narrow", "wide", None, None, None),
        P("narrow", "wide", None, None),
        P("narrow", "wide"),
    )
    return jax.shard_map(
        local,
        mesh=mesh,
        in_specs=placed,
        out_specs=(P(None, "narrow", "wide"), P()),
        check_vma=False,
    )
```

```python
import jax
import jax.numpy as jnp
import ml_dtypes
import numpy as np
from jax import lax
from jax.experimental import pallas as pl
from jax.experimental.pallas import tpu as pltpu
from jax.sharding import PartitionSpec as P

H = 128
TILE = 512
R = 256
HALF = R // 2
MODES = 4
BATCHES = 3
POS = 2
MESH = pl.DeviceIdType.MESH
F32 = jnp.float32
BF16 = jnp.bfloat16

PARTS = 3
CHUNKS = 16
ROWS = 24
ORDER = ((0, 1, 2), (1, 2, 0), (2, 0, 1))
STEPS = (1, 2, 3)


def tables():
    k = np.arange(R)
    angle = 2.0 * np.pi * ((np.arange(HALF)[:, None] * k[None, :]) % R) / R
    upper = np.cos(angle)
    lower = np.sin(angle)
    lower[0] = np.where(k % 2 == 0, 1.0, -1.0)
    packed = (np.concatenate([upper, lower]) / np.sqrt(R)).astype(np.float32)
    order = np.concatenate([np.arange(HALF), [HALF], R - np.arange(1, HALF)])
    select = np.zeros((R, R), np.float32)
    select[np.arange(R), order] = 1.0

    def pair(value):
        high = value.astype(ml_dtypes.bfloat16)
        low = (value - high.astype(np.float32)).astype(ml_dtypes.bfloat16)
        return [high, low]

    pick = select.astype(ml_dtypes.bfloat16)
    return np.stack(pair(packed) + pair(packed.T.copy()) + [pick, pick.T.copy()])


def split(value):
    high = value.astype(BF16)
    return high, (value - high.astype(F32)).astype(BF16)


def dot(a, b):
    return jnp.dot(a, b, preferred_element_type=F32)


def left_product(table, value):
    high, low = split(value)
    return dot(table[0], high) + dot(table[0], low) + dot(table[1], high)


def right_product(value, table):
    high, low = split(value)
    return dot(high, table[0]) + dot(low, table[0]) + dot(high, table[1])


def row_mask(shape):
    return lax.broadcasted_iota(jnp.int32, shape, 0) == 0


def rows_fixed(first, general):
    top = jnp.where(row_mask(first[:8].shape), first[:8], general[:8])
    return jnp.concatenate([top, general[8:]], axis=0)


def butterfly(zr, zi):
    ur, vr, ui, vi = zr[:HALF], zr[HALF:], zi[:HALF], zi[HALF:]
    plus = (rows_fixed(ur, ur + vi), rows_fixed(ui, ui - vr))
    minus = (rows_fixed(vr, ur - vi), rows_fixed(vi, ui + vr))
    first = lax.broadcasted_iota(jnp.int32, (HALF, HALF), 1) == 0
    out = []
    for re, im in (plus, minus):
        ur, vr, ui, vi = re[:, :HALF], re[:, HALF:], im[:, :HALF], im[:, HALF:]
        mr, mi = jnp.where(first, 0.0, vr), jnp.where(first, 0.0, vi)
        out.append(
            (
                (ur + mi, ui - mr),
                (jnp.where(first, vr, ur - vi), jnp.where(first, vi, ui + vr)),
            )
        )
    return out


def butterfly_transposed(quads):
    first = lax.broadcasted_iota(jnp.int32, (HALF, HALF), 1) == 0
    sides = []
    for (pr, pi), (qr, qi) in quads:
        ur = pr + jnp.where(first, 0.0, qr)
        ui = pi + jnp.where(first, 0.0, qi)
        vr = jnp.where(first, qr, qi - pi)
        vi = jnp.where(first, qi, pr - qr)
        sides.append((jnp.concatenate([ur, vr], axis=1), jnp.concatenate([ui, vi], axis=1)))
    (pr, pi), (qr, qi) = sides
    ur = rows_fixed(pr, pr + qr)
    ui = rows_fixed(pi, pi + qi)
    vr = rows_fixed(qr, qi - pi)
    vi = rows_fixed(qi, pr - qr)
    return jnp.concatenate([ur, vr, ui, vi], axis=0)


def read_plane(ref, plane):
    if plane == 3:
        value = ref[pl.ds(2 * CHUNKS, CHUNKS), pl.ds(0, 16), :]
        return value.reshape(R, R)
    start, stop = plane * R, (plane + 1) * R
    low, high = start // ROWS, -(-stop // ROWS)
    value = ref[pl.ds(low, high - low)].reshape((high - low) * ROWS, R)
    return value[start - low * ROWS : stop - low * ROWS]


def write_plane(ref, plane, value):
    if plane == 3:
        for chunk in range(CHUNKS):
            ref[2 * CHUNKS + chunk, pl.ds(0, 16), :] = value[16 * chunk : 16 * chunk + 16]
        return
    for tile in range(R // 8):
        row = plane * R + 8 * tile
        ref[row // ROWS, pl.ds(row % ROWS, 8), :] = value[8 * tile : 8 * tile + 8]


def whole_kernel(
    offs, cnt, obj, probe, patterns, tabs,
    obj_out, probe_out,
    pad, pbuf, gbuf, spat, patch, far, og, zbuf, grad, cover,
    acc0, acc1, recv0, recv1, recv2, cross, hside, hvert, hcorn,
    bsend, brecv, hsend, hrecv, gsend, grecv,
):
    wide = lax.axis_index("wide")
    x = lax.axis_index("narrow")
    n_wide = lax.axis_size("wide")
    n_narrow = lax.axis_size("narrow")
    core = wide % 2
    z = (wide // 2) % 4
    y = wide // 8
    place = (x, y, z)
    table = (tabs.at[0], tabs.at[1])
    table_t = (tabs.at[2], tabs.at[3])

    def device(at, c):
        return ((at[1] * 4 + at[2]) * 2 + c, at[0])

    def peer(dim, step):
        at = list(place)
        at[dim] = (at[dim] + step) % 4
        return device(at, core)

    sibling = device(place, 1 - core)

    left, right, above, below = ways = ((-1, 0), (1, 0), (0, -1), (0, 1))

    def there(way):
        if way[0]:
            return (wide > 0) if way[0] < 0 else (wide < n_wide - 1)
        return (x > 0) if way[1] < 0 else (x < n_narrow - 1)

    def away(way):
        return (wide + way[0], x + way[1])

    def back(way):
        return (-way[0], -way[1])

    for at in range(2):
        for lane in (0, 5):
            pad[at, lane] = jnp.zeros((TILE + 2 * H, H), F32)
        for lane in range(1, 5):
            pad[at, lane, pl.ds(0, H), :] = jnp.zeros((H, H), F32)
            pad[at, lane, pl.ds(H + TILE, H), :] = jnp.zeros((H, H), F32)
    hside[...] = jnp.zeros_like(hside)
    hvert[...] = jnp.zeros_like(hvert)

    barrier = pltpu.get_barrier_semaphore()
    pl.semaphore_signal(barrier, inc=1, device_id=sibling, device_id_type=MESH)
    for dim in range(3):
        for step in STEPS:
            pl.semaphore_signal(barrier, inc=1, device_id=peer(dim, step), device_id_type=MESH)
    total = 10
    for way in ways:
        total = total + there(way).astype(jnp.int32)

        @pl.when(there(way))
        def _():
            pl.semaphore_signal(barrier, inc=1, device_id=away(way), device_id_type=MESH)

    pl.semaphore_wait(barrier, total)

    def neighbour_copy(source, target, send_sem, recv_sem, index, way):
        return pltpu.make_async_remote_copy(
            src_ref=source,
            dst_ref=target,
            send_sem=send_sem.at[index],
            recv_sem=recv_sem.at[index],
            device_id=away(way),
            device_id_type=MESH,
        )

    def halo(index):
        if index < 2:
            way = ways[index]
            lane_from, lane_to = ((0, 5), (3, 0))[index]
            source = obj.at[:, :, pl.ds(lane_from * H, H)]
            return way, True, neighbour_copy(
                source, pad.at[:, lane_to, pl.ds(H, TILE), :], hsend, hrecv, index, way
            )
        if index < 10:
            lane = (0, 3, 1, 2)[(index - 2) // 2]
            side = (index - 2) % 2
            row_from, row_to = ((0, H + TILE), (TILE - H, 0))[side]
            source = obj.at[:, pl.ds(row_from, H), pl.ds(lane * H, H)]
            return ways[2 + side], True, neighbour_copy(
                source, pad.at[:, lane + 1, pl.ds(row_to, H), :], hsend, hrecv, index, ways[2 + side]
            )
        vertical, side = divmod(index - 10, 2)
        lane_from, lane_to = ((1, 5), (4, 0))[side]
        rows = pl.ds(vertical * (H + TILE), H)
        return ways[side], there(ways[2 + vertical]), neighbour_copy(
            pad.at[:, lane_from, rows, :], pad.at[:, lane_to, rows, :], hsend, hrecv, index, ways[side]
        )

    def both_there(way, also):
        return there(way) if also is True else jnp.logical_and(there(way), also)

    def start_if(copy):
        way, also, one = copy

        @pl.when(both_there(way, also))
        def _():
            one.start()

    def wait_send_if(copy):
        way, also, one = copy

        @pl.when(both_there(way, also))
        def _():
            one.wait_send()

    def wait_recv_if(copy):
        way, also, one = copy

        @pl.when(both_there(back(way), also))
        def _():
            one.wait_recv()

    for index in range(2, 10):
        start_if(halo(index))
    for index in range(2):
        start_if(halo(index))

    for at in range(2):
        for lane in range(4):
            pad[at, lane + 1, pl.ds(H, TILE), :] = obj[at, :, pl.ds(lane * H, H)]
    for half in range(2):
        for plane in range(4):
            write_plane(pbuf.at[0, half], plane, probe[half * 2 + plane // 2, plane % 2])
        for chunk in range(CHUNKS):
            pbuf[0, half, 2 * CHUNKS + chunk, pl.ds(16, 8), :] = jnp.zeros((8, R), F32)
    zbuf[...] = jnp.zeros_like(zbuf)
    grad[...] = jnp.zeros_like(grad)

    @pl.loop(0, BATCHES * POS)
    def _(slot):
        high, low = split(jnp.sqrt(patterns[slot]))
        high, low = split(dot(tabs[4], high) + dot(tabs[4], low))
        spat[slot] = dot(high, tabs[5]) + dot(low, tabs[5])

    for index in range(2, 6):
        wait_recv_if(halo(index))
    for index in range(10, 14):
        start_if(halo(index))
    for index in (0, 1, 6, 7, 8, 9, 10, 11, 12, 13):
        wait_recv_if(halo(index))
    for index in range(14):
        wait_send_if(halo(index))

    lanes = lax.broadcasted_iota(jnp.int32, (R, H), 1)

    def window(slot):
        row = offs[2 * slot] + H
        col = offs[2 * slot + 1] + H
        first = jnp.minimum(col // H, 3)
        return row, first, col - first * H

    def take_patches(batch):
        covered = jnp.zeros((8, R), F32)
        for position in range(POS):
            slot = batch * POS + position
            row, first, shift = window(slot)
            live = slot < cnt[0]
            turn = (H - shift) % H
            for at in range(2):
                turned = [
                    pltpu.roll(pad[at, first + k, pl.ds(row, R), :], turn, 1) for k in range(3)
                ]
                for k in range(2):
                    value = jnp.where(lanes < H - shift, turned[k], turned[k + 1])
                    value = jnp.where(live, value, 0.0)
                    patch[position, at, :, pl.ds(k * H, H)] = value
                    covered = covered + jnp.sum(value * value)
        cover[...] = covered

    take_patches(0)

    def half_planes(ref, mode):
        return read_plane(ref, 2 * mode), read_plane(ref, 2 * mode + 1)

    def run_batch(batch):
        for half in range(2):
            for chunk in range(CHUNKS):
                gbuf[half, 2 * CHUNKS + chunk, pl.ds(16, 8), :] = cover[...]

        @pl.loop(0, 2)
        def _(turn):
            half = (core + turn) % 2

            @pl.when(jnp.logical_and(turn == 1, batch > 0))
            def _():
                all_reduce_end(batch - 1)

            for mode in range(2):
                pr, pi = half_planes(pbuf.at[batch, half], mode)
                for position in range(POS):
                    our, oui = patch[position, 0], patch[position, 1]
                    psi = jnp.concatenate([pr * our - pi * oui, pr * oui + pi * our], axis=1)
                    left = left_product((table[0][...], table[1][...]), psi)
                    left = jnp.concatenate([left[:, :R], left[:, R:]], axis=0)
                    both = right_product(left, (table_t[0][...], table_t[1][...]))
                    quads = butterfly(both[:R], both[R:])
                    slot = half * 2 + mode
                    for a in range(2):
                        for b in range(2):
                            for at in range(2):
                                far[position, slot, at, pl.ds(a * HALF, HALF), pl.ds(b * HALF, HALF)] = (
                                    quads[a][b][at]
                                )

        for position in range(POS):

            @pl.loop(0, R // 32)
            def _(tile):
                rows = pl.ds(pl.multiple_of(tile * 32, 32), 32)
                power = jnp.zeros((32, R), F32)
                for mode in range(MODES):
                    re, im = far[position, mode, 0, rows, :], far[position, mode, 1, rows, :]
                    power = power + re * re + im * im
                slot = batch * POS + position
                spat[slot, rows, :] = 1.0 - spat[slot, rows, :] * lax.rsqrt(power + 0.1)

        @pl.loop(0, 2)
        def _(turn):
            half = (core + 1 + turn) % 2
            for mode in range(2):
                pr, pi = half_planes(pbuf.at[batch, half], mode)
                sum_re, sum_im = None, None
                for position in range(POS):
                    slot = half * 2 + mode
                    quads = []
                    for a in range(2):
                        row = []
                        for b in range(2):
                            rows, cols = pl.ds(a * HALF, HALF), pl.ds(b * HALF, HALF)
                            keep = spat[batch * POS + position, rows, cols]
                            row.append(
                                (
                                    far[position, slot, 0, rows, cols] * keep,
                                    far[position, slot, 1, rows, cols] * keep,
                                )
                            )
                        quads.append(row)
                    both = butterfly_transposed(quads)
                    right = right_product(both, (table[0][...], table[1][...]))
                    right = jnp.concatenate([right[:R], right[R:]], axis=1)
                    back = left_product((table_t[0][...], table_t[1][...]), right)
                    dr, di = back[:, :R], back[:, R:]
                    our, oui = patch[position, 0], patch[position, 1]
                    og_re = pr * dr + pi * di
                    og_im = pr * di - pi * dr
                    if mode == 0:

                        @pl.when(turn == 0)
                        def _():
                            og[position, 0] = og_re
                            og[position, 1] = og_im

                        @pl.when(turn != 0)
                        def _():
                            og[position, 0] += og_re
                            og[position, 1] += og_im
                    else:
                        og[position, 0] += og_re
                        og[position, 1] += og_im
                    pg_re = our * dr + oui * di
                    pg_im = our * di - oui * dr
                    sum_re = pg_re if sum_re is None else sum_re + pg_re
                    sum_im = pg_im if sum_im is None else sum_im + pg_im
                write_plane(gbuf.at[half], 2 * mode, sum_re)
                write_plane(gbuf.at[half], 2 * mode + 1, sum_im)

            @pl.when(turn == 0)
            def _():
                for part in range(PARTS):
                    to_sibling(batch, part).start()

    def add_gradient(batch):
        rows, firsts = [], []
        for position in range(POS):
            row, first, shift = window(batch * POS + position)
            rows.append(row)
            firsts.append(first)
            turn = shift % H
            for at in range(2):
                low = pltpu.roll(og[position, at, :, pl.ds(0, H)], turn, 1)
                high = pltpu.roll(og[position, at, :, pl.ds(H, H)], turn, 1)
                zbuf[position, at, 1, pl.ds(8, R), :] = jnp.where(lanes >= shift, low, 0.0)
                zbuf[position, at, 2, pl.ds(8, R), :] = jnp.where(lanes >= shift, high, low)
                zbuf[position, at, 3, pl.ds(8, R), :] = jnp.where(lanes >= shift, 0.0, high)

        @pl.loop(0, (TILE + 2 * H) // 16)
        def _(tile):
            base = pl.multiple_of(tile * 16, 16)
            for sub in range(2):
                at_row = base + 8 * sub
                starts = [jnp.clip(at_row - row + 8, 0, R + 8) for row in rows]
                for at in range(2):
                    for lane in range(6):
                        value = grad[at, lane, pl.ds(at_row, 8), :]
                        for position in range(POS):
                            source = jnp.clip(lane - firsts[position] + 1, 0, 4)
                            value = value + zbuf[position, at, source, pl.ds(starts[position], 8), :]
                        grad[at, lane, pl.ds(at_row, 8), :] = value

    def border_copy(index):
        if index < 4:
            vertical, side = divmod(index, 2)
            rows = pl.ds(vertical * (H + TILE), H)
            return ways[side], True, neighbour_copy(
                grad.at[:, (0, 5)[side], rows, :], hcorn.at[vertical, side], gsend, grecv, index, ways[side]
            )
        if index < 6:
            side = index - 4
            return ways[side], True, neighbour_copy(
                grad.at[:, (0, 5)[side], pl.ds(H, TILE), :], hside.at[side], gsend, grecv, index, ways[side]
            )
        lane = (1, 2, 0, 3)[(index - 6) // 2]
        vertical = (index - 6) % 2
        rows = pl.ds(vertical * (H + TILE), H)
        return ways[2 + vertical], True, neighbour_copy(
            grad.at[:, lane + 1, rows, :], hvert.at[vertical, :, lane], gsend, grecv, index, ways[2 + vertical]
        )

    def pass_corners():
        for index in range(4):
            vertical, side = divmod(index, 2)
            rows = pl.ds(vertical * (H + TILE), H)
            lane = (4, 1)[side]
            way, _, one = border_copy(index)

            @pl.when(there(back(way)))
            def _():
                one.wait_recv()
                for at in range(2):
                    grad[at, lane, rows, :] += hcorn[vertical, side, at]

        for index in range(10, 14):
            start_if(border_copy(index))

    def to_sibling(batch, part):
        span = pl.ds(part * CHUNKS, CHUNKS)
        return pltpu.make_async_remote_copy(
            src_ref=gbuf.at[1 - core, span],
            dst_ref=recv0.at[batch, span],
            send_sem=bsend.at[part],
            recv_sem=brecv.at[batch, part],
            device_id=sibling,
            device_id_type=MESH,
        )

    def shared(batch, part, step):
        chunk = part * CHUNKS + 4 * ((place[ORDER[part][0]] + 4 - step) % 4)
        group = pl.ds(chunk, 4)
        index = part * 4 + step

        def copy(half):
            ref = pbuf.at[batch + 1, half, group]
            return pltpu.make_async_remote_copy(
                src_ref=ref,
                dst_ref=ref,
                send_sem=bsend.at[3 + index],
                recv_sem=brecv.at[batch, 3 + index],
                device_id=sibling,
                device_id_type=MESH,
            )

        return copy

    def all_reduce_end(batch):
        for step in range(4):
            for part in range(PARTS):
                shared(batch, part, step)(1 - core).wait_recv()
                shared(batch, part, step)(core).wait_send()

    def all_reduce(batch):
        new = pbuf.at[batch + 1]
        old = pbuf.at[batch]

        def copy(source, target, index, to, send=0):
            return pltpu.make_async_remote_copy(
                src_ref=source,
                dst_ref=target,
                send_sem=bsend.at[send],
                recv_sem=brecv.at[batch, index],
                device_id=to,
                device_id_type=MESH,
            )

        sent = []

        def send(source, target, index, to):
            one = copy(source, target, index, to, 15 + len(sent))
            one.start()
            sent.append(one)

        def first_at(part, order):
            return (place[ORDER[part][1]] + 1 + order) % 4

        for part in range(PARTS):
            span = pl.ds(part * CHUNKS, CHUNKS)
            d1 = ORDER[part][0]
            to_sibling(batch, part).wait_recv()
            acc0[span] = gbuf[core, span] + recv0[batch, span]
            for order in range(4):
                for step in STEPS:
                    chunk = part * CHUNKS + 4 * ((place[d1] + step) % 4) + first_at(part, order)
                    target = recv1.at[batch, part, order, step - 1]
                    send(acc0.at[chunk], target, 15 + part * 4 + order, peer(d1, step))

        take_patches(jnp.minimum(batch + 1, BATCHES - 1))

        lasts = []
        for order in range(4):
            for part in range(PARTS):
                d1, d2, _ = ORDER[part]
                quarter = recv1.at[batch, part, order]
                copy(acc0.at[pl.ds(0, 3)], quarter, 15 + part * 4 + order, peer(d1, 1)).wait_recv()
                value = acc0[part * CHUNKS + 4 * place[d1] + first_at(part, order)]
                for step in STEPS:
                    value = value + quarter[step - 1]
                if order == 3:
                    lasts.append(value)
                else:
                    acc1[part, order] = value
                    target = recv2.at[batch, part, order]
                    send(acc1.at[part, order], target, 27 + part, peer(d2, order + 1))

        for part in range(PARTS):
            acc1[part, 3] = lasts[part]
        add_gradient(batch)

        @pl.when(batch == BATCHES - 1)
        def _():
            for index in range(10):
                start_if(border_copy(index))

        for part in range(PARTS):
            _, d2, d3 = ORDER[part]
            copy(acc1.at[part, pl.ds(0, 3)], recv2.at[batch, part], 27 + part, peer(d2, 1)).wait_recv()
            value = acc1[part, 3]
            for step in STEPS:
                value = value + recv2[batch, part, step - 1]
            cross[batch, part, place[d3]] = value
            for step in STEPS:
                mine = cross.at[batch, part, place[d3]]
                send(mine, mine, 30 + part * 3 + step - 1, peer(d3, step))

        @pl.when(batch == BATCHES - 1)
        def _():
            pass_corners()

        sums = []
        for part in range(PARTS):
            d3 = ORDER[part][2]
            for step in STEPS:
                theirs = cross.at[batch, part, (place[d3] + 4 - step) % 4]
                copy(theirs, theirs, 30 + part * 3 + step - 1, peer(d3, step)).wait_recv()
            value = cross[batch, part, 0]
            for at in range(1, 4):
                value = value + cross[batch, part, at]
            sums.append(value)
        scale = sums[2][16:] / float(R * R)
        scale = jnp.concatenate([scale, scale, scale], axis=0)

        def gather(part, chunk):
            d1 = ORDER[part][0]
            ref = new.at[core, chunk]
            for step in STEPS:
                send(ref, ref, 48 + part * 3 + step - 1, peer(d1, step))

        chunks = []
        for part in range(PARTS):
            d1, d2, _ = ORDER[part]
            chunk = part * CHUNKS + 4 * place[d1] + place[d2]
            chunks.append(chunk)
            new[core, chunk] = old[core, chunk] - sums[part] / scale
            for step in STEPS:
                mine = new.at[core, chunk]
                send(mine, mine, 39 + part * 3 + step - 1, peer(d2, step))
        for part in range(PARTS):
            gather(part, chunks[part])
        for step in (1, 3, 2):
            for part in range(PARTS):
                d1, d2, _ = ORDER[part]
                chunk = part * CHUNKS + 4 * place[d1] + (place[d2] + 4 - step) % 4
                theirs = new.at[core, chunk]
                copy(theirs, theirs, 39 + part * 3 + step - 1, peer(d2, step)).wait_recv()
                gather(part, chunk)
        for part in range(PARTS):
            shared(batch, part, 0)(core).start()
        for step in (1, 3, 2):
            for part in range(PARTS):
                d1 = ORDER[part][0]
                group = new.at[core, pl.ds(part * CHUNKS + 4 * ((place[d1] + 4 - step) % 4), 4)]
                copy(group, group, 48 + part * 3 + step - 1, peer(d1, step)).wait_recv()
                shared(batch, part, step)(core).start()
        for part in range(PARTS):
            to_sibling(batch, part).wait_send()
        for one in sent:
            one.wait_send()

    @pl.loop(0, BATCHES)
    def _(batch):
        run_batch(batch)
        all_reduce(batch)

    all_reduce_end(BATCHES - 1)

    power = jnp.zeros((R, R), F32)
    for half in range(2):
        for plane in range(4):
            value = read_plane(pbuf.at[BATCHES, half], plane)
            probe_out[half * 2 + plane // 2, plane % 2] = value
            power = power + value * value
    top = jnp.max(power)

    for index in range(4, 14):
        wait_recv_if(border_copy(index))
    for index in range(14):
        wait_send_if(border_copy(index))

    def came(lane, row, rows, at):
        value = grad[at, lane + 1, pl.ds(H + row, rows), :]
        if lane == 0:
            value = value + hside[1, at, pl.ds(row, rows), :]
        if lane == 3:
            value = value + hside[0, at, pl.ds(row, rows), :]
        if row == 0:
            value = value + hvert[1, at, lane]
        if row == TILE - H:
            value = value + hvert[0, at, lane]
        return value

    for at in range(2):
        for lane in range(4):
            for row in range(0, TILE, H):
                place_at = (at, pl.ds(row, H), pl.ds(lane * H, H))
                obj_out[place_at] = obj[place_at] - 0.5 * came(lane, row, H, at) / top


def local(object_field, probe, patterns, offsets, counts):
    vmem = pl.BlockSpec(memory_space=pltpu.VMEM)
    smem = pl.BlockSpec(memory_space=pltpu.SMEM)
    dma = pltpu.SemaphoreType.DMA
    return pl.pallas_call(
        whole_kernel,
        out_shape=(
            jax.ShapeDtypeStruct((2, TILE, TILE), F32),
            jax.ShapeDtypeStruct((MODES, 2, R, R), F32),
        ),
        in_specs=[smem, smem, vmem, vmem, vmem, vmem],
        out_specs=(vmem, vmem),
        scratch_shapes=[
            pltpu.VMEM((2, 6, TILE + 2 * H, H), F32),
            pltpu.VMEM((BATCHES + 1, 2, PARTS * CHUNKS, ROWS, R), F32),
            pltpu.VMEM((2, PARTS * CHUNKS, ROWS, R), F32),
            pltpu.VMEM((BATCHES * POS, R, R), F32),
            pltpu.VMEM((POS, 2, R, R), F32),
            pltpu.VMEM((POS, MODES, 2, R, R), F32),
            pltpu.VMEM((POS, 2, R, R), F32),
            pltpu.VMEM((POS, 2, 5, R + 16, H), F32),
            pltpu.VMEM((2, 6, TILE + 2 * H, H), F32),
            pltpu.VMEM((8, R), F32),
            pltpu.VMEM((PARTS * CHUNKS, ROWS, R), F32),
            pltpu.VMEM((PARTS, 4, ROWS, R), F32),
            pltpu.VMEM((BATCHES, PARTS * CHUNKS, ROWS, R), F32),
            pltpu.VMEM((BATCHES, PARTS, 4, 3, ROWS, R), F32),
            pltpu.VMEM((BATCHES, PARTS, 3, ROWS, R), F32),
            pltpu.VMEM((BATCHES, PARTS, 4, ROWS, R), F32),
            pltpu.VMEM((2, 2, TILE, H), F32),
            pltpu.VMEM((2, 2, 4, H, H), F32),
            pltpu.VMEM((2, 2, 2, H, H), F32),
            dma((114,)),
            dma((BATCHES, 57)),
            dma((14,)),
            dma((14,)),
            dma((14,)),
            dma((14,)),
        ],
        compiler_params=pltpu.CompilerParams(
            collective_id=0, has_side_effects=True, vmem_limit_bytes=67043328
        ),
    )(
        offsets.reshape(BATCHES * POS * 2),
        counts.reshape(1),
        object_field,
        probe,
        patterns.reshape(BATCHES * POS, R, R),
        jnp.asarray(tables()),
    )


def solution(mesh):
    placed = (
        P(None, "narrow", "wide"),
        P(),
        P("narrow", "wide", None, None, None),
        P("narrow", "wide", None, None),
        P("narrow", "wide"),
    )
    return jax.shard_map(
        local,
        mesh=mesh,
        in_specs=placed,
        out_specs=(P(None, "narrow", "wide"), P()),
        check_vma=False,
    )
```

```python
import jax
import jax.numpy as jnp
import ml_dtypes
import numpy as np
from jax import lax
from jax.experimental import pallas as pl
from jax.experimental.pallas import tpu as pltpu
from jax.sharding import PartitionSpec as P

H = 128
TILE = 512
R = 256
HALF = R // 2
MODES = 4
BATCHES = 3
POS = 2
MESH = pl.DeviceIdType.MESH
F32 = jnp.float32
BF16 = jnp.bfloat16

PARTS = 3
CHUNKS = 16
ROWS = 24
ORDER = ((0, 1, 2), (1, 2, 0), (2, 0, 1))
STEPS = (2, 1, 3)


def tables():
    k = np.arange(R)
    angle = 2.0 * np.pi * ((np.arange(HALF)[:, None] * k[None, :]) % R) / R
    upper = np.cos(angle)
    lower = np.sin(angle)
    lower[0] = np.where(k % 2 == 0, 1.0, -1.0)
    packed = (np.concatenate([upper, lower]) / np.sqrt(R)).astype(np.float32)
    order = np.concatenate([np.arange(HALF), [HALF], R - np.arange(1, HALF)])
    select = np.zeros((R, R), np.float32)
    select[np.arange(R), order] = 1.0

    def pair(value):
        high = value.astype(ml_dtypes.bfloat16)
        low = (value - high.astype(np.float32)).astype(ml_dtypes.bfloat16)
        return [high, low]

    pick = select.astype(ml_dtypes.bfloat16)
    return np.stack(pair(packed) + pair(packed.T.copy()) + [pick, pick.T.copy()])


def split(value):
    high = value.astype(BF16)
    return high, (value - high.astype(F32)).astype(BF16)


def dot(a, b):
    return jnp.dot(a, b, preferred_element_type=F32)


def left_product(table, value):
    high, low = split(value)
    return dot(table[0], high) + dot(table[0], low) + dot(table[1], high)


def right_product(value, table):
    high, low = split(value)
    return dot(high, table[0]) + dot(low, table[0]) + dot(high, table[1])


def row_mask(shape):
    return lax.broadcasted_iota(jnp.int32, shape, 0) == 0


def rows_fixed(first, general):
    top = jnp.where(row_mask(first[:8].shape), first[:8], general[:8])
    return jnp.concatenate([top, general[8:]], axis=0)


def butterfly(zr, zi):
    ur, vr, ui, vi = zr[:HALF], zr[HALF:], zi[:HALF], zi[HALF:]
    plus = (rows_fixed(ur, ur + vi), rows_fixed(ui, ui - vr))
    minus = (rows_fixed(vr, ur - vi), rows_fixed(vi, ui + vr))
    first = lax.broadcasted_iota(jnp.int32, (HALF, HALF), 1) == 0
    out = []
    for re, im in (plus, minus):
        ur, vr, ui, vi = re[:, :HALF], re[:, HALF:], im[:, :HALF], im[:, HALF:]
        mr, mi = jnp.where(first, 0.0, vr), jnp.where(first, 0.0, vi)
        out.append(
            (
                (ur + mi, ui - mr),
                (jnp.where(first, vr, ur - vi), jnp.where(first, vi, ui + vr)),
            )
        )
    return out


def butterfly_transposed(quads):
    first = lax.broadcasted_iota(jnp.int32, (HALF, HALF), 1) == 0
    sides = []
    for (pr, pi), (qr, qi) in quads:
        ur = pr + jnp.where(first, 0.0, qr)
        ui = pi + jnp.where(first, 0.0, qi)
        vr = jnp.where(first, qr, qi - pi)
        vi = jnp.where(first, qi, pr - qr)
        sides.append((jnp.concatenate([ur, vr], axis=1), jnp.concatenate([ui, vi], axis=1)))
    (pr, pi), (qr, qi) = sides
    ur = rows_fixed(pr, pr + qr)
    ui = rows_fixed(pi, pi + qi)
    vr = rows_fixed(qr, qi - pi)
    vi = rows_fixed(qi, pr - qr)
    return jnp.concatenate([ur, vr, ui, vi], axis=0)


def read_plane(ref, plane):
    if plane == 3:
        value = ref[pl.ds(2 * CHUNKS, CHUNKS), pl.ds(0, 16), :]
        return value.reshape(R, R)
    start, stop = plane * R, (plane + 1) * R
    low, high = start // ROWS, -(-stop // ROWS)
    value = ref[pl.ds(low, high - low)].reshape((high - low) * ROWS, R)
    return value[start - low * ROWS : stop - low * ROWS]


def write_plane(ref, plane, value):
    if plane == 3:
        for chunk in range(CHUNKS):
            ref[2 * CHUNKS + chunk, pl.ds(0, 16), :] = value[16 * chunk : 16 * chunk + 16]
        return
    for tile in range(R // 8):
        row = plane * R + 8 * tile
        ref[row // ROWS, pl.ds(row % ROWS, 8), :] = value[8 * tile : 8 * tile + 8]


def whole_kernel(
    offs, cnt, obj, probe_in, patterns_in, tabs_in,
    obj_out, probe_out,
    probe, tabs, pad, pbuf, gbuf, spat, patch, far, og, zbuf, grad, cover,
    acc0, acc1, recv0, recv1, recv2, cross, hside, hvert, hcorn,
    load, bsend, brecv, hsend, hrecv, gsend, grecv,
):
    wide = lax.axis_index("wide")
    x = lax.axis_index("narrow")
    n_wide = lax.axis_size("wide")
    n_narrow = lax.axis_size("narrow")
    core = wide % 2
    z = (wide // 2) % 4
    y = wide // 8
    place = (x, y, z)
    table = (tabs.at[0], tabs.at[1])
    table_t = (tabs.at[2], tabs.at[3])

    def device(at, c):
        return ((at[1] * 4 + at[2]) * 2 + c, at[0])

    def peer(dim, step):
        at = list(place)
        at[dim] = (at[dim] + step) % 4
        return device(at, core)

    sibling = device(place, 1 - core)

    left, right, above, below = ways = ((-1, 0), (1, 0), (0, -1), (0, 1))

    def there(way):
        if way[0]:
            return (wide > 0) if way[0] < 0 else (wide < n_wide - 1)
        return (x > 0) if way[1] < 0 else (x < n_narrow - 1)

    def away(way):
        return (wide + way[0], x + way[1])

    def back(way):
        return (-way[0], -way[1])

    loads = [
        pltpu.make_async_copy(source, target, load.at[index])
        for index, (source, target) in enumerate(
            ((tabs_in, tabs), (patterns_in, spat), (probe_in, probe))
        )
    ]
    for one in loads:
        one.start()

    barrier = pltpu.get_barrier_semaphore()
    pl.semaphore_signal(barrier, inc=1, device_id=sibling, device_id_type=MESH)
    for dim in range(3):
        for step in STEPS:
            pl.semaphore_signal(barrier, inc=1, device_id=peer(dim, step), device_id_type=MESH)
    total = 10
    for way in ways:
        total = total + there(way).astype(jnp.int32)

        @pl.when(there(way))
        def _():
            pl.semaphore_signal(barrier, inc=1, device_id=away(way), device_id_type=MESH)

    pl.semaphore_wait(barrier, total)

    def neighbour_copy(source, target, send_sem, recv_sem, index, way):
        return pltpu.make_async_remote_copy(
            src_ref=source,
            dst_ref=target,
            send_sem=send_sem.at[index],
            recv_sem=recv_sem.at[index],
            device_id=away(way),
            device_id_type=MESH,
        )

    def halo(index):
        if index < 2:
            way = ways[index]
            lane_from, lane_to = ((0, 5), (3, 0))[index]
            source = obj.at[:, :, pl.ds(lane_from * H, H)]
            return way, True, neighbour_copy(
                source, pad.at[:, lane_to, pl.ds(H, TILE), :], hsend, hrecv, index, way
            )
        if index < 10:
            lane = (0, 3, 1, 2)[(index - 2) // 2]
            side = (index - 2) % 2
            row_from, row_to = ((0, H + TILE), (TILE - H, 0))[side]
            source = obj.at[:, pl.ds(row_from, H), pl.ds(lane * H, H)]
            return ways[2 + side], True, neighbour_copy(
                source, pad.at[:, lane + 1, pl.ds(row_to, H), :], hsend, hrecv, index, ways[2 + side]
            )
        vertical, side = divmod(index - 10, 2)
        lane_from, lane_to = ((1, 5), (4, 0))[side]
        rows = pl.ds(vertical * (H + TILE), H)
        return ways[side], there(ways[2 + vertical]), neighbour_copy(
            pad.at[:, lane_from, rows, :], pad.at[:, lane_to, rows, :], hsend, hrecv, index, ways[side]
        )

    def both_there(way, also):
        return there(way) if also is True else jnp.logical_and(there(way), also)

    def start_if(copy):
        way, also, one = copy

        @pl.when(both_there(way, also))
        def _():
            one.start()

    def wait_send_if(copy):
        way, also, one = copy

        @pl.when(both_there(way, also))
        def _():
            one.wait_send()

    def wait_recv_if(copy):
        way, also, one = copy

        @pl.when(both_there(back(way), also))
        def _():
            one.wait_recv()

    for index in range(2, 10):
        start_if(halo(index))
    for index in range(2):
        start_if(halo(index))

    for side in range(2):
        lane = (0, 5)[side]

        @pl.when(jnp.logical_not(there(ways[side])))
        def _():
            for at in range(2):
                pad[at, lane, pl.ds(H, TILE), :] = jnp.zeros((TILE, H), F32)
            hside[1 - side] = jnp.zeros((2, TILE, H), F32)

        for vertical in range(2):

            @pl.when(jnp.logical_not(jnp.logical_and(there(ways[side]), there(ways[2 + vertical]))))
            def _():
                for at in range(2):
                    pad[at, lane, pl.ds(vertical * (H + TILE), H), :] = jnp.zeros((H, H), F32)

    for vertical in range(2):

        @pl.when(jnp.logical_not(there(ways[2 + vertical])))
        def _():
            for at in range(2):
                for lane in range(1, 5):
                    pad[at, lane, pl.ds(vertical * (H + TILE), H), :] = jnp.zeros((H, H), F32)
            hvert[1 - vertical] = jnp.zeros((2, 4, H, H), F32)

    for at in range(2):
        for lane in range(4):
            pad[at, lane + 1, pl.ds(H, TILE), :] = obj[at, :, pl.ds(lane * H, H)]
    for one in loads:
        one.wait()
    for half in range(2):
        for plane in range(4):
            write_plane(pbuf.at[0, half], plane, probe[half * 2 + plane // 2, plane % 2])
        for chunk in range(CHUNKS):
            pbuf[0, half, 2 * CHUNKS + chunk, pl.ds(16, 8), :] = jnp.zeros((8, R), F32)
    zbuf[...] = jnp.zeros_like(zbuf)
    grad[...] = jnp.zeros_like(grad)

    @pl.loop(0, BATCHES * POS)
    def _(slot):
        high, low = split(jnp.sqrt(spat[slot]))
        high, low = split(dot(tabs[4], high) + dot(tabs[4], low))
        spat[slot] = dot(high, tabs[5]) + dot(low, tabs[5])

    for index in range(2, 6):
        wait_recv_if(halo(index))
    for index in range(10, 14):
        start_if(halo(index))
    for index in (0, 1, 6, 7, 8, 9, 10, 11, 12, 13):
        wait_recv_if(halo(index))
    for index in range(14):
        wait_send_if(halo(index))

    lanes = lax.broadcasted_iota(jnp.int32, (R, H), 1)

    def window(slot):
        row = offs[0, slot] + H
        col = offs[1, slot] + H
        first = jnp.minimum(col // H, 3)
        return row, first, col - first * H

    def take_patches(batch):
        covered = jnp.zeros((8, R), F32)
        for position in range(POS):
            slot = batch * POS + position
            row, first, shift = window(slot)
            live = slot < cnt[0]
            turn = (H - shift) % H
            for at in range(2):
                turned = [
                    pltpu.roll(pad[at, first + k, pl.ds(row, R), :], turn, 1) for k in range(3)
                ]
                for k in range(2):
                    value = jnp.where(lanes < H - shift, turned[k], turned[k + 1])
                    value = jnp.where(live, value, 0.0)
                    patch[position, at, :, pl.ds(k * H, H)] = value
                    covered = covered + jnp.sum(value * value)
        cover[...] = covered

    take_patches(0)

    def half_planes(ref, mode):
        return read_plane(ref, 2 * mode), read_plane(ref, 2 * mode + 1)

    def run_batch(batch):
        for half in range(2):
            for chunk in range(CHUNKS):
                gbuf[half, 2 * CHUNKS + chunk, pl.ds(16, 8), :] = cover[...]

        @pl.loop(0, 2)
        def _(turn):
            half = (core + turn) % 2

            @pl.when(jnp.logical_and(turn == 1, batch > 0))
            def _():
                all_reduce_end(batch - 1)

            for mode in range(2):
                pr, pi = half_planes(pbuf.at[batch, half], mode)
                for position in range(POS):
                    our, oui = patch[position, 0], patch[position, 1]
                    psi = jnp.concatenate([pr * our - pi * oui, pr * oui + pi * our], axis=1)
                    left = left_product((table[0][...], table[1][...]), psi)
                    left = jnp.concatenate([left[:, :R], left[:, R:]], axis=0)
                    both = right_product(left, (table_t[0][...], table_t[1][...]))
                    quads = butterfly(both[:R], both[R:])
                    slot = half * 2 + mode
                    for a in range(2):
                        for b in range(2):
                            for at in range(2):
                                far[position, slot, at, pl.ds(a * HALF, HALF), pl.ds(b * HALF, HALF)] = (
                                    quads[a][b][at]
                                )

        for position in range(POS):

            @pl.loop(0, R // 32)
            def _(tile):
                rows = pl.ds(pl.multiple_of(tile * 32, 32), 32)
                power = jnp.zeros((32, R), F32)
                for mode in range(MODES):
                    re, im = far[position, mode, 0, rows, :], far[position, mode, 1, rows, :]
                    power = power + re * re + im * im
                slot = batch * POS + position
                spat[slot, rows, :] = 1.0 - spat[slot, rows, :] * lax.rsqrt(power + 0.1)

        @pl.loop(0, 2)
        def _(turn):
            half = (core + 1 + turn) % 2
            grads = [[jnp.where(turn == 0, 0.0, og[p, at]) for at in range(2)] for p in range(POS)]
            for mode in range(2):
                pr, pi = half_planes(pbuf.at[batch, half], mode)
                sum_re, sum_im = None, None
                for position in range(POS):
                    slot = half * 2 + mode
                    quads = []
                    for a in range(2):
                        row = []
                        for b in range(2):
                            rows, cols = pl.ds(a * HALF, HALF), pl.ds(b * HALF, HALF)
                            keep = spat[batch * POS + position, rows, cols]
                            row.append(
                                (
                                    far[position, slot, 0, rows, cols] * keep,
                                    far[position, slot, 1, rows, cols] * keep,
                                )
                            )
                        quads.append(row)
                    both = butterfly_transposed(quads)
                    right = right_product(both, (table[0][...], table[1][...]))
                    right = jnp.concatenate([right[:R], right[R:]], axis=1)
                    back = left_product((table_t[0][...], table_t[1][...]), right)
                    dr, di = back[:, :R], back[:, R:]
                    our, oui = patch[position, 0], patch[position, 1]
                    og_re = pr * dr + pi * di
                    og_im = pr * di - pi * dr
                    grads[position][0] += og_re
                    grads[position][1] += og_im
                    pg_re = our * dr + oui * di
                    pg_im = our * di - oui * dr
                    sum_re = pg_re if sum_re is None else sum_re + pg_re
                    sum_im = pg_im if sum_im is None else sum_im + pg_im
                write_plane(gbuf.at[half], 2 * mode, sum_re)
                write_plane(gbuf.at[half], 2 * mode + 1, sum_im)
            for p in range(POS):
                for at in range(2):
                    og[p, at] = grads[p][at]

            @pl.when(turn == 0)
            def _():
                for part in range(PARTS):
                    to_sibling(batch, part).start()

    def add_gradient(batch):
        rows, firsts = [], []
        for position in range(POS):
            row, first, shift = window(batch * POS + position)
            rows.append(row)
            firsts.append(first)
            turn = shift % H
            for at in range(2):
                low = pltpu.roll(og[position, at, :, pl.ds(0, H)], turn, 1)
                high = pltpu.roll(og[position, at, :, pl.ds(H, H)], turn, 1)
                zbuf[position, at, 1, pl.ds(8, R), :] = jnp.where(lanes >= shift, low, 0.0)
                zbuf[position, at, 2, pl.ds(8, R), :] = jnp.where(lanes >= shift, high, low)
                zbuf[position, at, 3, pl.ds(8, R), :] = jnp.where(lanes >= shift, 0.0, high)

        @pl.loop(0, (TILE + 2 * H) // 16)
        def _(tile):
            base = pl.multiple_of(tile * 16, 16)
            for sub in range(2):
                at_row = base + 8 * sub
                starts = [jnp.clip(at_row - row + 8, 0, R + 8) for row in rows]
                for at in range(2):
                    for lane in range(6):
                        value = grad[at, lane, pl.ds(at_row, 8), :]
                        for position in range(POS):
                            source = jnp.clip(lane - firsts[position] + 1, 0, 4)
                            value = value + zbuf[position, at, source, pl.ds(starts[position], 8), :]
                        grad[at, lane, pl.ds(at_row, 8), :] = value

    def border_copy(index):
        if index < 4:
            vertical, side = divmod(index, 2)
            rows = pl.ds(vertical * (H + TILE), H)
            return ways[side], True, neighbour_copy(
                grad.at[:, (0, 5)[side], rows, :], hcorn.at[vertical, side], gsend, grecv, index, ways[side]
            )
        if index < 12:
            piece, side = divmod(index - 4, 2)
            return ways[side], True, neighbour_copy(
                grad.at[:, (0, 5)[side], pl.ds(H + H * piece, H), :],
                hside.at[side, :, pl.ds(H * piece, H), :],
                gsend, grecv, index, ways[side],
            )
        lane = (1, 2, 0, 3)[(index - 12) // 2]
        vertical = (index - 12) % 2
        rows = pl.ds(vertical * (H + TILE), H)
        return ways[2 + vertical], True, neighbour_copy(
            grad.at[:, lane + 1, rows, :], hvert.at[vertical, :, lane], gsend, grecv, index, ways[2 + vertical]
        )

    def pass_corners():
        for index in range(4):
            vertical, side = divmod(index, 2)
            rows = pl.ds(vertical * (H + TILE), H)
            lane = (4, 1)[side]
            way, _, one = border_copy(index)

            @pl.when(there(back(way)))
            def _():
                one.wait_recv()
                for at in range(2):
                    grad[at, lane, rows, :] += hcorn[vertical, side, at]

    def border_turn(batch, turn):
        @pl.when(batch == BATCHES - 1)
        def _():
            if turn == 0:
                for index in range(4):
                    start_if(border_copy(index))
            if turn == 2:
                pass_corners()
            for index in (2 * turn + 12, 2 * turn + 13, 2 * turn + 4, 2 * turn + 5):
                start_if(border_copy(index))

    def to_sibling(batch, part):
        span = pl.ds(part * CHUNKS, CHUNKS)
        return pltpu.make_async_remote_copy(
            src_ref=gbuf.at[1 - core, span],
            dst_ref=recv0.at[batch, span],
            send_sem=bsend.at[part],
            recv_sem=brecv.at[batch, part],
            device_id=sibling,
            device_id_type=MESH,
        )

    def shared(batch, part, step):
        chunk = part * CHUNKS + 4 * ((place[ORDER[part][0]] + 4 - step) % 4)
        group = pl.ds(chunk, 4)
        index = part * 4 + step

        def copy(half):
            ref = pbuf.at[batch + 1, half, group]
            return pltpu.make_async_remote_copy(
                src_ref=ref,
                dst_ref=ref,
                send_sem=bsend.at[3 + index],
                recv_sem=brecv.at[batch, 3 + index],
                device_id=sibling,
                device_id_type=MESH,
            )

        return copy

    def all_reduce_end(batch):
        for step in range(4):
            for part in range(PARTS):
                shared(batch, part, step)(1 - core).wait_recv()
                shared(batch, part, step)(core).wait_send()

    def all_reduce(batch):
        new = pbuf.at[batch + 1]
        old = pbuf.at[batch]

        def copy(source, target, index, to, send=0):
            return pltpu.make_async_remote_copy(
                src_ref=source,
                dst_ref=target,
                send_sem=bsend.at[send],
                recv_sem=brecv.at[batch, index],
                device_id=to,
                device_id_type=MESH,
            )

        sent = []

        def send(source, target, index, to):
            one = copy(source, target, index, to, 15 + len(sent))
            one.start()
            sent.append(one)

        def first_at(part, order):
            return (place[ORDER[part][1]] + 1 + order) % 4

        for part in range(PARTS):
            span = pl.ds(part * CHUNKS, CHUNKS)
            d1 = ORDER[part][0]
            to_sibling(batch, part).wait_recv()
            acc0[span] = gbuf[core, span] + recv0[batch, span]
            for order in range(4):
                for step in STEPS:
                    chunk = part * CHUNKS + 4 * ((place[d1] + step) % 4) + first_at(part, order)
                    target = recv1.at[batch, part, order, step - 1]
                    send(acc0.at[chunk], target, 15 + part * 4 + order, peer(d1, step))

        add_gradient(batch)
        border_turn(batch, 0)

        lasts = []
        for order in range(4):
            for part in range(PARTS):
                d1, d2, _ = ORDER[part]
                quarter = recv1.at[batch, part, order]
                copy(acc0.at[pl.ds(0, 3)], quarter, 15 + part * 4 + order, peer(d1, 1)).wait_recv()
                value = acc0[part * CHUNKS + 4 * place[d1] + first_at(part, order)]
                for step in STEPS:
                    value = value + quarter[step - 1]
                if order == 3:
                    lasts.append(value)
                else:
                    acc1[part, order] = value
                    target = recv2.at[batch, part, order]
                    send(acc1.at[part, order], target, 27 + part, peer(d2, order + 1))

        for part in range(PARTS):
            acc1[part, 3] = lasts[part]
        border_turn(batch, 1)

        @pl.when(batch < BATCHES - 1)
        def _():
            take_patches(batch + 1)

        for part in range(PARTS):
            _, d2, d3 = ORDER[part]
            copy(acc1.at[part, pl.ds(0, 3)], recv2.at[batch, part], 27 + part, peer(d2, 1)).wait_recv()
            value = acc1[part, 3]
            for step in STEPS:
                value = value + recv2[batch, part, step - 1]
            cross[batch, part, place[d3]] = value
            for step in STEPS:
                mine = cross.at[batch, part, place[d3]]
                send(mine, mine, 30 + part * 3 + step - 1, peer(d3, step))

        border_turn(batch, 2)
        sums = []
        for part in range(PARTS):
            d3 = ORDER[part][2]
            for step in STEPS:
                theirs = cross.at[batch, part, (place[d3] + 4 - step) % 4]
                copy(theirs, theirs, 30 + part * 3 + step - 1, peer(d3, step)).wait_recv()
            value = cross[batch, part, 0]
            for at in range(1, 4):
                value = value + cross[batch, part, at]
            sums.append(value)
        scale = sums[2][16:] / float(R * R)
        scale = jnp.concatenate([scale, scale, scale], axis=0)

        def gather(part, chunk):
            d1 = ORDER[part][0]
            ref = new.at[core, chunk]
            for step in STEPS:
                send(ref, ref, 48 + part * 3 + step - 1, peer(d1, step))

        chunks = []
        for part in range(PARTS):
            d1, d2, _ = ORDER[part]
            chunk = part * CHUNKS + 4 * place[d1] + place[d2]
            chunks.append(chunk)
            new[core, chunk] = old[core, chunk] - sums[part] / scale
            for step in STEPS:
                mine = new.at[core, chunk]
                send(mine, mine, 39 + part * 3 + step - 1, peer(d2, step))
        for part in range(PARTS):
            gather(part, chunks[part])
        border_turn(batch, 3)
        for step in (1, 3, 2):
            for part in range(PARTS):
                d1, d2, _ = ORDER[part]
                chunk = part * CHUNKS + 4 * place[d1] + (place[d2] + 4 - step) % 4
                theirs = new.at[core, chunk]
                copy(theirs, theirs, 39 + part * 3 + step - 1, peer(d2, step)).wait_recv()
                gather(part, chunk)
        for part in range(PARTS):
            shared(batch, part, 0)(core).start()
        for step in (1, 3, 2):
            for part in range(PARTS):
                d1 = ORDER[part][0]
                group = new.at[core, pl.ds(part * CHUNKS + 4 * ((place[d1] + 4 - step) % 4), 4)]
                copy(group, group, 48 + part * 3 + step - 1, peer(d1, step)).wait_recv()
                shared(batch, part, step)(core).start()
        for part in range(PARTS):
            to_sibling(batch, part).wait_send()
        for one in sent:
            one.wait_send()

    @pl.loop(0, BATCHES)
    def _(batch):
        run_batch(batch)
        all_reduce(batch)

    all_reduce_end(BATCHES - 1)

    power = jnp.zeros((R, R), F32)
    for half in range(2):
        for plane in range(4):
            value = read_plane(pbuf.at[BATCHES, half], plane)
            probe_out[half * 2 + plane // 2, plane % 2] = value
            power = power + value * value
    top = jnp.max(power)

    for index in range(4, 20):
        wait_recv_if(border_copy(index))
    for index in range(20):
        wait_send_if(border_copy(index))

    def came(lane, row, rows, at):
        value = grad[at, lane + 1, pl.ds(H + row, rows), :]
        if lane == 0:
            value = value + hside[1, at, pl.ds(row, rows), :]
        if lane == 3:
            value = value + hside[0, at, pl.ds(row, rows), :]
        if row == 0:
            value = value + hvert[1, at, lane]
        if row == TILE - H:
            value = value + hvert[0, at, lane]
        return value

    for at in range(2):
        for lane in range(4):
            for row in range(0, TILE, H):
                place_at = (at, pl.ds(row, H), pl.ds(lane * H, H))
                obj_out[place_at] = obj[place_at] - 0.5 * came(lane, row, H, at) / top


def local(object_field, probe, patterns, offsets, counts):
    vmem = pl.BlockSpec(memory_space=pltpu.VMEM)
    hbm = pl.BlockSpec(memory_space=pltpu.HBM)
    smem = pl.BlockSpec(memory_space=pltpu.SMEM)
    dma = pltpu.SemaphoreType.DMA
    return pl.pallas_call(
        whole_kernel,
        out_shape=(
            pltpu.VMEM((2, TILE, TILE), F32),
            pltpu.VMEM((MODES, 2, R, R), F32),
        ),
        in_specs=[smem, smem, vmem, hbm, hbm, hbm],
        out_specs=(vmem, vmem),
        scratch_shapes=[
            pltpu.VMEM((MODES, 2, R, R), F32),
            pltpu.VMEM((6, R, R), BF16),
            pltpu.VMEM((2, 6, TILE + 2 * H, H), F32),
            pltpu.VMEM((BATCHES + 1, 2, PARTS * CHUNKS, ROWS, R), F32),
            pltpu.VMEM((2, PARTS * CHUNKS, ROWS, R), F32),
            pltpu.VMEM((BATCHES * POS, R, R), F32),
            pltpu.VMEM((POS, 2, R, R), F32),
            pltpu.VMEM((POS, MODES, 2, R, R), F32),
            pltpu.VMEM((POS, 2, R, R), F32),
            pltpu.VMEM((POS, 2, 5, R + 16, H), F32),
            pltpu.VMEM((2, 6, TILE + 2 * H, H), F32),
            pltpu.VMEM((8, R), F32),
            pltpu.VMEM((PARTS * CHUNKS, ROWS, R), F32),
            pltpu.VMEM((PARTS, 4, ROWS, R), F32),
            pltpu.VMEM((BATCHES, PARTS * CHUNKS, ROWS, R), F32),
            pltpu.VMEM((BATCHES, PARTS, 4, 3, ROWS, R), F32),
            pltpu.VMEM((BATCHES, PARTS, 3, ROWS, R), F32),
            pltpu.VMEM((BATCHES, PARTS, 4, ROWS, R), F32),
            pltpu.VMEM((2, 2, TILE, H), F32),
            pltpu.VMEM((2, 2, 4, H, H), F32),
            pltpu.VMEM((2, 2, 2, H, H), F32),
            dma((3,)),
            dma((114,)),
            dma((BATCHES, 57)),
            dma((14,)),
            dma((14,)),
            dma((20,)),
            dma((20,)),
        ],
        compiler_params=pltpu.CompilerParams(
            collective_id=0, has_side_effects=True, vmem_limit_bytes=56 * 1024 * 1024
        ),
    )(
        offsets.reshape(BATCHES * POS, 2).T,
        counts.reshape(1),
        object_field,
        probe,
        patterns.reshape(BATCHES * POS, R, R),
        jnp.asarray(tables()),
    )


def solution(mesh):
    placed = (
        P(None, "narrow", "wide"),
        P(),
        P("narrow", "wide", None, None, None),
        P("narrow", "wide", None, None),
        P("narrow", "wide"),
    )
    return jax.shard_map(
        local,
        mesh=mesh,
        in_specs=placed,
        out_specs=(P(None, "narrow", "wide"), P()),
        check_vma=False,
    )
```

```python
import jax
import jax.numpy as jnp
import ml_dtypes
import numpy as np
from jax import lax
from jax.experimental import pallas as pl
from jax.experimental.pallas import tpu as pltpu
from jax.sharding import PartitionSpec as P

H = 128
TILE = 512
R = 256
HALF = R // 2
MODES = 4
BATCHES = 3
POS = 2
MESH = pl.DeviceIdType.MESH
F32 = jnp.float32
BF16 = jnp.bfloat16

PARTS = 3
CHUNKS = 16
ROWS = 24
ORDER = ((0, 1, 2), (1, 2, 0), (2, 0, 1))
STEPS = (2, 1, 3)


def tables():
    k = np.arange(R)
    angle = 2.0 * np.pi * ((np.arange(HALF)[:, None] * k[None, :]) % R) / R
    upper = np.cos(angle)
    lower = np.sin(angle)
    lower[0] = np.where(k % 2 == 0, 1.0, -1.0)
    packed = (np.concatenate([upper, lower]) / np.sqrt(R)).astype(np.float32)
    order = np.concatenate([np.arange(HALF), [HALF], R - np.arange(1, HALF)])
    select = np.zeros((R, R), np.float32)
    select[np.arange(R), order] = 1.0

    def pair(value):
        high = value.astype(ml_dtypes.bfloat16)
        low = (value - high.astype(np.float32)).astype(ml_dtypes.bfloat16)
        return [high, low]

    pick = select.astype(ml_dtypes.bfloat16)
    return np.stack(pair(packed) + pair(packed.T.copy()) + [pick, pick.T.copy()])


def split(value):
    high = value.astype(BF16)
    return high, (value - high.astype(F32)).astype(BF16)


def dot(a, b):
    return jnp.dot(a, b, preferred_element_type=F32)


def left_product(table, value):
    high, low = split(value)
    return dot(table[0], high) + dot(table[0], low) + dot(table[1], high)


def right_product(value, table):
    high, low = split(value)
    return dot(high, table[0]) + dot(low, table[0]) + dot(high, table[1])


def row_mask(shape):
    return lax.broadcasted_iota(jnp.int32, shape, 0) == 0


def rows_fixed(first, general):
    top = jnp.where(row_mask(first[:8].shape), first[:8], general[:8])
    return jnp.concatenate([top, general[8:]], axis=0)


def butterfly(zr, zi):
    ur, vr, ui, vi = zr[:HALF], zr[HALF:], zi[:HALF], zi[HALF:]
    plus = (rows_fixed(ur, ur + vi), rows_fixed(ui, ui - vr))
    minus = (rows_fixed(vr, ur - vi), rows_fixed(vi, ui + vr))
    first = lax.broadcasted_iota(jnp.int32, (HALF, HALF), 1) == 0
    out = []
    for re, im in (plus, minus):
        ur, vr, ui, vi = re[:, :HALF], re[:, HALF:], im[:, :HALF], im[:, HALF:]
        mr, mi = jnp.where(first, 0.0, vr), jnp.where(first, 0.0, vi)
        out.append(
            (
                (ur + mi, ui - mr),
                (jnp.where(first, vr, ur - vi), jnp.where(first, vi, ui + vr)),
            )
        )
    return out


def butterfly_transposed(quads):
    first = lax.broadcasted_iota(jnp.int32, (HALF, HALF), 1) == 0
    sides = []
    for (pr, pi), (qr, qi) in quads:
        ur = pr + jnp.where(first, 0.0, qr)
        ui = pi + jnp.where(first, 0.0, qi)
        vr = jnp.where(first, qr, qi - pi)
        vi = jnp.where(first, qi, pr - qr)
        sides.append((jnp.concatenate([ur, vr], axis=1), jnp.concatenate([ui, vi], axis=1)))
    (pr, pi), (qr, qi) = sides
    ur = rows_fixed(pr, pr + qr)
    ui = rows_fixed(pi, pi + qi)
    vr = rows_fixed(qr, qi - pi)
    vi = rows_fixed(qi, pr - qr)
    return jnp.concatenate([ur, vr, ui, vi], axis=0)


def read_plane(ref, plane):
    if plane == 3:
        value = ref[pl.ds(2 * CHUNKS, CHUNKS), pl.ds(0, 16), :]
        return value.reshape(R, R)
    start, stop = plane * R, (plane + 1) * R
    low, high = start // ROWS, -(-stop // ROWS)
    value = ref[pl.ds(low, high - low)].reshape((high - low) * ROWS, R)
    return value[start - low * ROWS : stop - low * ROWS]


def write_plane(ref, plane, value):
    if plane == 3:
        for chunk in range(CHUNKS):
            ref[2 * CHUNKS + chunk, pl.ds(0, 16), :] = value[16 * chunk : 16 * chunk + 16]
        return
    for tile in range(R // 8):
        row = plane * R + 8 * tile
        ref[row // ROWS, pl.ds(row % ROWS, 8), :] = value[8 * tile : 8 * tile + 8]


def whole_kernel(
    offs, cnt, obj_in, probe_in, patterns_in, tabs_in,
    obj_out, probe_out,
    obj, probe, tabs, pad, pbuf, gbuf, spat, patch, far, og, zbuf, grad, cover,
    acc0, acc1, recv0, recv1, recv2, cross, hside, hvert, hcorn,
    load, bsend, brecv, hsend, hrecv, gsend, grecv,
):
    wide = lax.axis_index("wide")
    x = lax.axis_index("narrow")
    n_wide = lax.axis_size("wide")
    n_narrow = lax.axis_size("narrow")
    core = wide % 2
    z = (wide // 2) % 4
    y = wide // 8
    place = (x, y, z)
    table = (tabs.at[0], tabs.at[1])
    table_t = (tabs.at[2], tabs.at[3])

    def device(at, c):
        return ((at[1] * 4 + at[2]) * 2 + c, at[0])

    def peer(dim, step):
        at = list(place)
        at[dim] = (at[dim] + step) % 4
        return device(at, core)

    sibling = device(place, 1 - core)

    left, right, above, below = ways = ((-1, 0), (1, 0), (0, -1), (0, 1))

    def there(way):
        if way[0]:
            return (wide > 0) if way[0] < 0 else (wide < n_wide - 1)
        return (x > 0) if way[1] < 0 else (x < n_narrow - 1)

    def away(way):
        return (wide + way[0], x + way[1])

    def back(way):
        return (-way[0], -way[1])

    loads = [
        pltpu.make_async_copy(source, target, load.at[index])
        for index, (source, target) in enumerate(
            ((obj_in, obj), (tabs_in, tabs), (patterns_in, spat), (probe_in, probe))
        )
    ]
    for one in loads:
        one.start()

    barrier = pltpu.get_barrier_semaphore()
    pl.semaphore_signal(barrier, inc=1, device_id=sibling, device_id_type=MESH)
    for dim in range(3):
        for step in STEPS:
            pl.semaphore_signal(barrier, inc=1, device_id=peer(dim, step), device_id_type=MESH)
    total = 10
    for way in ways:
        total = total + there(way).astype(jnp.int32)

        @pl.when(there(way))
        def _():
            pl.semaphore_signal(barrier, inc=1, device_id=away(way), device_id_type=MESH)

    pl.semaphore_wait(barrier, total)
    loads[0].wait()

    def neighbour_copy(source, target, send_sem, recv_sem, index, way):
        return pltpu.make_async_remote_copy(
            src_ref=source,
            dst_ref=target,
            send_sem=send_sem.at[index],
            recv_sem=recv_sem.at[index],
            device_id=away(way),
            device_id_type=MESH,
        )

    def halo(index):
        if index < 2:
            way = ways[index]
            lane_from, lane_to = ((0, 5), (3, 0))[index]
            source = obj.at[:, :, pl.ds(lane_from * H, H)]
            return way, True, neighbour_copy(
                source, pad.at[:, lane_to, pl.ds(H, TILE), :], hsend, hrecv, index, way
            )
        if index < 10:
            lane = (0, 3, 1, 2)[(index - 2) // 2]
            side = (index - 2) % 2
            row_from, row_to = ((0, H + TILE), (TILE - H, 0))[side]
            source = obj.at[:, pl.ds(row_from, H), pl.ds(lane * H, H)]
            return ways[2 + side], True, neighbour_copy(
                source, pad.at[:, lane + 1, pl.ds(row_to, H), :], hsend, hrecv, index, ways[2 + side]
            )
        vertical, side = divmod(index - 10, 2)
        lane_from, lane_to = ((1, 5), (4, 0))[side]
        rows = pl.ds(vertical * (H + TILE), H)
        return ways[side], there(ways[2 + vertical]), neighbour_copy(
            pad.at[:, lane_from, rows, :], pad.at[:, lane_to, rows, :], hsend, hrecv, index, ways[side]
        )

    def both_there(way, also):
        return there(way) if also is True else jnp.logical_and(there(way), also)

    def start_if(copy):
        way, also, one = copy

        @pl.when(both_there(way, also))
        def _():
            one.start()

    def wait_send_if(copy):
        way, also, one = copy

        @pl.when(both_there(way, also))
        def _():
            one.wait_send()

    def wait_recv_if(copy):
        way, also, one = copy

        @pl.when(both_there(back(way), also))
        def _():
            one.wait_recv()

    for index in range(2, 10):
        start_if(halo(index))
    for index in range(2):
        start_if(halo(index))

    for side in range(2):
        lane = (0, 5)[side]

        @pl.when(jnp.logical_not(there(ways[side])))
        def _():
            for at in range(2):
                pad[at, lane, pl.ds(H, TILE), :] = jnp.zeros((TILE, H), F32)
            hside[1 - side] = jnp.zeros((2, TILE, H), F32)

        for vertical in range(2):

            @pl.when(jnp.logical_not(jnp.logical_and(there(ways[side]), there(ways[2 + vertical]))))
            def _():
                for at in range(2):
                    pad[at, lane, pl.ds(vertical * (H + TILE), H), :] = jnp.zeros((H, H), F32)

    for vertical in range(2):

        @pl.when(jnp.logical_not(there(ways[2 + vertical])))
        def _():
            for at in range(2):
                for lane in range(1, 5):
                    pad[at, lane, pl.ds(vertical * (H + TILE), H), :] = jnp.zeros((H, H), F32)
            hvert[1 - vertical] = jnp.zeros((2, 4, H, H), F32)

    for at in range(2):
        for lane in range(4):
            pad[at, lane + 1, pl.ds(H, TILE), :] = obj[at, :, pl.ds(lane * H, H)]
    for one in loads[1:]:
        one.wait()
    for half in range(2):
        for plane in range(4):
            write_plane(pbuf.at[0, half], plane, probe[half * 2 + plane // 2, plane % 2])
        for chunk in range(CHUNKS):
            pbuf[0, half, 2 * CHUNKS + chunk, pl.ds(16, 8), :] = jnp.zeros((8, R), F32)
    zbuf[...] = jnp.zeros_like(zbuf)
    grad[...] = jnp.zeros_like(grad)

    @pl.loop(0, BATCHES * POS)
    def _(slot):
        high, low = split(jnp.sqrt(spat[slot]))
        high, low = split(dot(tabs[4], high) + dot(tabs[4], low))
        spat[slot] = dot(high, tabs[5]) + dot(low, tabs[5])

    for index in range(2, 6):
        wait_recv_if(halo(index))
    for index in range(10, 14):
        start_if(halo(index))
    for index in (0, 1, 6, 7, 8, 9, 10, 11, 12, 13):
        wait_recv_if(halo(index))
    for index in range(14):
        wait_send_if(halo(index))

    lanes = lax.broadcasted_iota(jnp.int32, (R, H), 1)

    def window(slot):
        row = offs[0, slot] + H
        col = offs[1, slot] + H
        first = jnp.minimum(col // H, 3)
        return row, first, col - first * H

    def take_patches(batch):
        covered = jnp.zeros((8, R), F32)
        for position in range(POS):
            slot = batch * POS + position
            row, first, shift = window(slot)
            live = slot < cnt[0]
            turn = (H - shift) % H
            for at in range(2):
                turned = [
                    pltpu.roll(pad[at, first + k, pl.ds(row, R), :], turn, 1) for k in range(3)
                ]
                for k in range(2):
                    value = jnp.where(lanes < H - shift, turned[k], turned[k + 1])
                    value = jnp.where(live, value, 0.0)
                    patch[position, at, :, pl.ds(k * H, H)] = value
                    covered = covered + jnp.sum(value * value)
        cover[...] = covered

    take_patches(0)

    def half_planes(ref, mode):
        return read_plane(ref, 2 * mode), read_plane(ref, 2 * mode + 1)

    def run_batch(batch):
        for half in range(2):
            for chunk in range(CHUNKS):
                gbuf[half, 2 * CHUNKS + chunk, pl.ds(16, 8), :] = cover[...]

        @pl.loop(0, 2)
        def _(turn):
            half = (core + turn) % 2

            @pl.when(jnp.logical_and(turn == 1, batch > 0))
            def _():
                all_reduce_end(batch - 1)

            for mode in range(2):
                pr, pi = half_planes(pbuf.at[batch, half], mode)
                for position in range(POS):
                    our, oui = patch[position, 0], patch[position, 1]
                    psi = jnp.concatenate([pr * our - pi * oui, pr * oui + pi * our], axis=1)
                    left = left_product((table[0][...], table[1][...]), psi)
                    left = jnp.concatenate([left[:, :R], left[:, R:]], axis=0)
                    both = right_product(left, (table_t[0][...], table_t[1][...]))
                    quads = butterfly(both[:R], both[R:])
                    slot = half * 2 + mode
                    for a in range(2):
                        for b in range(2):
                            for at in range(2):
                                far[position, slot, at, pl.ds(a * HALF, HALF), pl.ds(b * HALF, HALF)] = (
                                    quads[a][b][at]
                                )

        for position in range(POS):
            for tile in range(R // 32):
                rows = pl.ds(tile * 32, 32)
                power = jnp.zeros((32, R), F32)
                for mode in range(MODES):
                    re, im = far[position, mode, 0, rows, :], far[position, mode, 1, rows, :]
                    power = power + re * re + im * im
                slot = batch * POS + position
                spat[slot, rows, :] = 1.0 - spat[slot, rows, :] * lax.rsqrt(power + 0.1)

        for turn in range(2):
            half = (core + 1 + turn) % 2
            for mode in range(2):
                pr, pi = half_planes(pbuf.at[batch, half], mode)
                sum_re, sum_im = None, None
                for position in range(POS):
                    slot = half * 2 + mode
                    quads = []
                    for a in range(2):
                        row = []
                        for b in range(2):
                            rows, cols = pl.ds(a * HALF, HALF), pl.ds(b * HALF, HALF)
                            keep = spat[batch * POS + position, rows, cols]
                            row.append(
                                (
                                    far[position, slot, 0, rows, cols] * keep,
                                    far[position, slot, 1, rows, cols] * keep,
                                )
                            )
                        quads.append(row)
                    both = butterfly_transposed(quads)
                    right = right_product(both, (table[0][...], table[1][...]))
                    right = jnp.concatenate([right[:R], right[R:]], axis=1)
                    back = left_product((table_t[0][...], table_t[1][...]), right)
                    dr, di = back[:, :R], back[:, R:]
                    our, oui = patch[position, 0], patch[position, 1]
                    og_re = pr * dr + pi * di
                    og_im = pr * di - pi * dr
                    if turn == 0 and mode == 0:
                        og[position, 0] = og_re
                        og[position, 1] = og_im
                    else:
                        og[position, 0] += og_re
                        og[position, 1] += og_im
                    pg_re = our * dr + oui * di
                    pg_im = our * di - oui * dr
                    sum_re = pg_re if sum_re is None else sum_re + pg_re
                    sum_im = pg_im if sum_im is None else sum_im + pg_im
                write_plane(gbuf.at[half], 2 * mode, sum_re)
                write_plane(gbuf.at[half], 2 * mode + 1, sum_im)
            if turn == 0:
                for part in range(PARTS):
                    to_sibling(batch, part).start()

    def add_gradient(batch):
        rows, firsts = [], []
        for position in range(POS):
            row, first, shift = window(batch * POS + position)
            rows.append(row)
            firsts.append(first)
            turn = shift % H
            for at in range(2):
                low = pltpu.roll(og[position, at, :, pl.ds(0, H)], turn, 1)
                high = pltpu.roll(og[position, at, :, pl.ds(H, H)], turn, 1)
                zbuf[position, at, 1, pl.ds(8, R), :] = jnp.where(lanes >= shift, low, 0.0)
                zbuf[position, at, 2, pl.ds(8, R), :] = jnp.where(lanes >= shift, high, low)
                zbuf[position, at, 3, pl.ds(8, R), :] = jnp.where(lanes >= shift, 0.0, high)

        @pl.loop(0, (TILE + 2 * H) // 16)
        def _(tile):
            base = pl.multiple_of(tile * 16, 16)
            for sub in range(2):
                at_row = base + 8 * sub
                starts = [jnp.clip(at_row - row + 8, 0, R + 8) for row in rows]
                for at in range(2):
                    for lane in range(6):
                        value = grad[at, lane, pl.ds(at_row, 8), :]
                        for position in range(POS):
                            source = jnp.clip(lane - firsts[position] + 1, 0, 4)
                            value = value + zbuf[position, at, source, pl.ds(starts[position], 8), :]
                        grad[at, lane, pl.ds(at_row, 8), :] = value

    def border_copy(index):
        if index < 4:
            vertical, side = divmod(index, 2)
            rows = pl.ds(vertical * (H + TILE), H)
            return ways[side], True, neighbour_copy(
                grad.at[:, (0, 5)[side], rows, :], hcorn.at[vertical, side], gsend, grecv, index, ways[side]
            )
        if index < 12:
            piece, side = divmod(index - 4, 2)
            return ways[side], True, neighbour_copy(
                grad.at[:, (0, 5)[side], pl.ds(H + H * piece, H), :],
                hside.at[side, :, pl.ds(H * piece, H), :],
                gsend, grecv, index, ways[side],
            )
        lane = (1, 2, 0, 3)[(index - 12) // 2]
        vertical = (index - 12) % 2
        rows = pl.ds(vertical * (H + TILE), H)
        return ways[2 + vertical], True, neighbour_copy(
            grad.at[:, lane + 1, rows, :], hvert.at[vertical, :, lane], gsend, grecv, index, ways[2 + vertical]
        )

    def pass_corners():
        for index in range(4):
            vertical, side = divmod(index, 2)
            rows = pl.ds(vertical * (H + TILE), H)
            lane = (4, 1)[side]
            way, _, one = border_copy(index)

            @pl.when(there(back(way)))
            def _():
                one.wait_recv()
                for at in range(2):
                    grad[at, lane, rows, :] += hcorn[vertical, side, at]

    def border_turn(batch, turn):
        @pl.when(batch == BATCHES - 1)
        def _():
            if turn == 0:
                for index in range(4):
                    start_if(border_copy(index))
            if turn == 2:
                pass_corners()
            for index in (2 * turn + 12, 2 * turn + 13, 2 * turn + 4, 2 * turn + 5):
                start_if(border_copy(index))

    def to_sibling(batch, part):
        span = pl.ds(part * CHUNKS, CHUNKS)
        return pltpu.make_async_remote_copy(
            src_ref=gbuf.at[1 - core, span],
            dst_ref=recv0.at[batch, span],
            send_sem=bsend.at[part],
            recv_sem=brecv.at[batch, part],
            device_id=sibling,
            device_id_type=MESH,
        )

    def shared(batch, part, step):
        chunk = part * CHUNKS + 4 * ((place[ORDER[part][0]] + 4 - step) % 4)
        group = pl.ds(chunk, 4)
        index = part * 4 + step

        def copy(half):
            ref = pbuf.at[batch + 1, half, group]
            return pltpu.make_async_remote_copy(
                src_ref=ref,
                dst_ref=ref,
                send_sem=bsend.at[3 + index],
                recv_sem=brecv.at[batch, 3 + index],
                device_id=sibling,
                device_id_type=MESH,
            )

        return copy

    def all_reduce_end(batch):
        for step in range(4):
            for part in range(PARTS):
                shared(batch, part, step)(1 - core).wait_recv()
                shared(batch, part, step)(core).wait_send()

    def all_reduce(batch):
        new = pbuf.at[batch + 1]
        old = pbuf.at[batch]

        def copy(source, target, index, to, send=0):
            return pltpu.make_async_remote_copy(
                src_ref=source,
                dst_ref=target,
                send_sem=bsend.at[send],
                recv_sem=brecv.at[batch, index],
                device_id=to,
                device_id_type=MESH,
            )

        sent = []

        def send(source, target, index, to):
            one = copy(source, target, index, to, 15 + len(sent))
            one.start()
            sent.append(one)

        def first_at(part, order):
            return (place[ORDER[part][1]] + 1 + order) % 4

        for part in range(PARTS):
            span = pl.ds(part * CHUNKS, CHUNKS)
            d1 = ORDER[part][0]
            to_sibling(batch, part).wait_recv()
            acc0[span] = gbuf[core, span] + recv0[batch, span]
            for order in range(4):
                for step in STEPS:
                    chunk = part * CHUNKS + 4 * ((place[d1] + step) % 4) + first_at(part, order)
                    target = recv1.at[batch, part, order, step - 1]
                    send(acc0.at[chunk], target, 15 + part * 4 + order, peer(d1, step))

        add_gradient(batch)
        border_turn(batch, 0)

        lasts = []
        for order in range(4):
            for part in range(PARTS):
                d1, d2, _ = ORDER[part]
                quarter = recv1.at[batch, part, order]
                copy(acc0.at[pl.ds(0, 3)], quarter, 15 + part * 4 + order, peer(d1, 1)).wait_recv()
                value = acc0[part * CHUNKS + 4 * place[d1] + first_at(part, order)]
                for step in STEPS:
                    value = value + quarter[step - 1]
                if order == 3:
                    lasts.append(value)
                else:
                    acc1[part, order] = value
                    target = recv2.at[batch, part, order]
                    send(acc1.at[part, order], target, 27 + part, peer(d2, order + 1))

        for part in range(PARTS):
            acc1[part, 3] = lasts[part]
        border_turn(batch, 1)

        @pl.when(batch < BATCHES - 1)
        def _():
            take_patches(batch + 1)

        for part in range(PARTS):
            _, d2, d3 = ORDER[part]
            copy(acc1.at[part, pl.ds(0, 3)], recv2.at[batch, part], 27 + part, peer(d2, 1)).wait_recv()
            value = acc1[part, 3]
            for step in STEPS:
                value = value + recv2[batch, part, step - 1]
            cross[batch, part, place[d3]] = value
            for step in STEPS:
                mine = cross.at[batch, part, place[d3]]
                send(mine, mine, 30 + part * 3 + step - 1, peer(d3, step))

        border_turn(batch, 2)
        sums = []
        for part in range(PARTS):
            d3 = ORDER[part][2]
            for step in STEPS:
                theirs = cross.at[batch, part, (place[d3] + 4 - step) % 4]
                copy(theirs, theirs, 30 + part * 3 + step - 1, peer(d3, step)).wait_recv()
            value = cross[batch, part, 0]
            for at in range(1, 4):
                value = value + cross[batch, part, at]
            sums.append(value)
        scale = sums[2][16:] / float(R * R)
        scale = jnp.concatenate([scale, scale, scale], axis=0)

        def gather(part, chunk):
            d1 = ORDER[part][0]
            ref = new.at[core, chunk]
            for step in STEPS:
                send(ref, ref, 48 + part * 3 + step - 1, peer(d1, step))

        chunks = []
        for part in range(PARTS):
            d1, d2, _ = ORDER[part]
            chunk = part * CHUNKS + 4 * place[d1] + place[d2]
            chunks.append(chunk)
            new[core, chunk] = old[core, chunk] - sums[part] / scale
            for step in STEPS:
                mine = new.at[core, chunk]
                send(mine, mine, 39 + part * 3 + step - 1, peer(d2, step))
        for part in range(PARTS):
            gather(part, chunks[part])
        border_turn(batch, 3)
        for step in (1, 3, 2):
            for part in range(PARTS):
                d1, d2, _ = ORDER[part]
                chunk = part * CHUNKS + 4 * place[d1] + (place[d2] + 4 - step) % 4
                theirs = new.at[core, chunk]
                copy(theirs, theirs, 39 + part * 3 + step - 1, peer(d2, step)).wait_recv()
                gather(part, chunk)
        for part in range(PARTS):
            shared(batch, part, 0)(core).start()
        for step in (1, 3, 2):
            for part in range(PARTS):
                d1 = ORDER[part][0]
                group = new.at[core, pl.ds(part * CHUNKS + 4 * ((place[d1] + 4 - step) % 4), 4)]
                copy(group, group, 48 + part * 3 + step - 1, peer(d1, step)).wait_recv()
                shared(batch, part, step)(core).start()
        for part in range(PARTS):
            to_sibling(batch, part).wait_send()
        for one in sent:
            one.wait_send()

    @pl.loop(0, BATCHES)
    def _(batch):
        run_batch(batch)
        all_reduce(batch)

    all_reduce_end(BATCHES - 1)

    power = jnp.zeros((R, R), F32)
    for half in range(2):
        for plane in range(4):
            value = read_plane(pbuf.at[BATCHES, half], plane)
            probe_out[half * 2 + plane // 2, plane % 2] = value
            power = power + value * value
    part_of_top = 0.5 / jnp.max(power)

    for index in range(4, 20):
        wait_recv_if(border_copy(index))
    for index in range(20):
        wait_send_if(border_copy(index))

    def came(lane, row, rows, at):
        value = grad[at, lane + 1, pl.ds(H + row, rows), :]
        if lane == 0:
            value = value + hside[1, at, pl.ds(row, rows), :]
        if lane == 3:
            value = value + hside[0, at, pl.ds(row, rows), :]
        if row == 0:
            value = value + hvert[1, at, lane]
        if row == TILE - H:
            value = value + hvert[0, at, lane]
        return value

    for at in range(2):
        for lane in range(4):
            for row in range(0, TILE, H):
                place_at = (at, pl.ds(row, H), pl.ds(lane * H, H))
                obj_out[place_at] = obj[place_at] - came(lane, row, H, at) * part_of_top


def ship_kernel(obj, probe, obj_out, probe_out, sems):
    copies = [
        pltpu.make_async_copy(obj, obj_out, sems.at[0]),
        pltpu.make_async_copy(probe, probe_out, sems.at[1]),
    ]
    for one in copies:
        one.start()
    for one in copies:
        one.wait()


def local(object_field, probe, patterns, offsets, counts):
    vmem = pl.BlockSpec(memory_space=pltpu.VMEM)
    hbm = pl.BlockSpec(memory_space=pltpu.HBM)
    smem = pl.BlockSpec(memory_space=pltpu.SMEM)
    dma = pltpu.SemaphoreType.DMA
    done = pl.pallas_call(
        whole_kernel,
        out_shape=(
            pltpu.VMEM((2, TILE, TILE), F32),
            pltpu.VMEM((MODES, 2, R, R), F32),
        ),
        in_specs=[smem, smem, hbm, hbm, hbm, hbm],
        out_specs=(vmem, vmem),
        scratch_shapes=[
            pltpu.VMEM((2, TILE, TILE), F32),
            pltpu.VMEM((MODES, 2, R, R), F32),
            pltpu.VMEM((6, R, R), BF16),
            pltpu.VMEM((2, 6, TILE + 2 * H, H), F32),
            pltpu.VMEM((BATCHES + 1, 2, PARTS * CHUNKS, ROWS, R), F32),
            pltpu.VMEM((2, PARTS * CHUNKS, ROWS, R), F32),
            pltpu.VMEM((BATCHES * POS, R, R), F32),
            pltpu.VMEM((POS, 2, R, R), F32),
            pltpu.VMEM((POS, MODES, 2, R, R), F32),
            pltpu.VMEM((POS, 2, R, R), F32),
            pltpu.VMEM((POS, 2, 5, R + 16, H), F32),
            pltpu.VMEM((2, 6, TILE + 2 * H, H), F32),
            pltpu.VMEM((8, R), F32),
            pltpu.VMEM((PARTS * CHUNKS, ROWS, R), F32),
            pltpu.VMEM((PARTS, 4, ROWS, R), F32),
            pltpu.VMEM((BATCHES, PARTS * CHUNKS, ROWS, R), F32),
            pltpu.VMEM((BATCHES, PARTS, 4, 3, ROWS, R), F32),
            pltpu.VMEM((BATCHES, PARTS, 3, ROWS, R), F32),
            pltpu.VMEM((BATCHES, PARTS, 4, ROWS, R), F32),
            pltpu.VMEM((2, 2, TILE, H), F32),
            pltpu.VMEM((2, 2, 4, H, H), F32),
            pltpu.VMEM((2, 2, 2, H, H), F32),
            dma((4,)),
            dma((114,)),
            dma((BATCHES, 57)),
            dma((14,)),
            dma((14,)),
            dma((20,)),
            dma((20,)),
        ],
        compiler_params=pltpu.CompilerParams(
            collective_id=0, has_side_effects=True, vmem_limit_bytes=56 * 1024 * 1024
        ),
    )(
        offsets.reshape(BATCHES * POS, 2).T,
        counts.reshape(1),
        object_field,
        probe,
        patterns.reshape(BATCHES * POS, R, R),
        jnp.asarray(tables()),
    )
    return pl.pallas_call(
        ship_kernel,
        out_shape=(
            jax.ShapeDtypeStruct((2, TILE, TILE), F32),
            jax.ShapeDtypeStruct((MODES, 2, R, R), F32),
        ),
        in_specs=[vmem, vmem],
        out_specs=(hbm, hbm),
        scratch_shapes=[dma((2,))],
        compiler_params=pltpu.CompilerParams(vmem_limit_bytes=1024 * 1024),
    )(*done)


def solution(mesh):
    placed = (
        P(None, "narrow", "wide"),
        P(),
        P("narrow", "wide", None, None, None),
        P("narrow", "wide", None, None),
        P("narrow", "wide"),
    )
    return jax.shard_map(
        local,
        mesh=mesh,
        in_specs=placed,
        out_specs=(P(None, "narrow", "wide"), P()),
        check_vma=False,
    )
```

```python
import jax
import jax.numpy as jnp
import ml_dtypes
import numpy as np
from jax import lax
from jax.experimental import pallas as pl
from jax.experimental.pallas import tpu as pltpu
from jax.sharding import PartitionSpec as P

H = 128
TILE = 512
R = 256
HALF = R // 2
MODES = 4
BATCHES = 3
POS = 2
MESH = pl.DeviceIdType.MESH
F32 = jnp.float32
BF16 = jnp.bfloat16

PARTS = 3
CHUNKS = 16
ROWS = 24
ORDER = ((1, 2, 0), (2, 0, 1), (0, 1, 2))
KEPT = (24, 24, 16)
STEPS = (2, 1, 3)


def tables():
    k = np.arange(R)
    angle = 2.0 * np.pi * ((np.arange(HALF)[:, None] * k[None, :]) % R) / R
    upper = np.cos(angle)
    lower = np.sin(angle)
    lower[0] = np.where(k % 2 == 0, 1.0, -1.0)
    packed = (np.concatenate([upper, lower]) / np.sqrt(R)).astype(np.float32)
    order = np.concatenate([np.arange(HALF), [HALF], R - np.arange(1, HALF)])
    select = np.zeros((R, R), np.float32)
    select[np.arange(R), order] = 1.0

    def pair(value):
        high = value.astype(ml_dtypes.bfloat16)
        low = (value - high.astype(np.float32)).astype(ml_dtypes.bfloat16)
        return [high, low]

    pick = select.astype(ml_dtypes.bfloat16)
    return np.stack(pair(packed) + pair(packed.T.copy()) + [pick, pick.T.copy()])


def split(value):
    high = value.astype(BF16)
    return high, (value - high.astype(F32)).astype(BF16)


def dot(a, b):
    return jnp.dot(a, b, preferred_element_type=F32)


def left_product(table, value):
    high, low = split(value)
    return dot(table[0], high) + dot(table[0], low) + dot(table[1], high)


def right_product(value, table):
    high, low = split(value)
    return dot(high, table[0]) + dot(low, table[0]) + dot(high, table[1])


def row_mask(shape):
    return lax.broadcasted_iota(jnp.int32, shape, 0) == 0


def rows_fixed(first, general):
    top = jnp.where(row_mask(first[:8].shape), first[:8], general[:8])
    return jnp.concatenate([top, general[8:]], axis=0)


def butterfly(zr, zi):
    ur, vr, ui, vi = zr[:HALF], zr[HALF:], zi[:HALF], zi[HALF:]
    plus = (rows_fixed(ur, ur + vi), rows_fixed(ui, ui - vr))
    minus = (rows_fixed(vr, ur - vi), rows_fixed(vi, ui + vr))
    first = lax.broadcasted_iota(jnp.int32, (HALF, HALF), 1) == 0
    out = []
    for re, im in (plus, minus):
        ur, vr, ui, vi = re[:, :HALF], re[:, HALF:], im[:, :HALF], im[:, HALF:]
        mr, mi = jnp.where(first, 0.0, vr), jnp.where(first, 0.0, vi)
        out.append(
            (
                (ur + mi, ui - mr),
                (jnp.where(first, vr, ur - vi), jnp.where(first, vi, ui + vr)),
            )
        )
    return out


def butterfly_transposed(quads):
    first = lax.broadcasted_iota(jnp.int32, (HALF, HALF), 1) == 0
    sides = []
    for (pr, pi), (qr, qi) in quads:
        ur = pr + jnp.where(first, 0.0, qr)
        ui = pi + jnp.where(first, 0.0, qi)
        vr = jnp.where(first, qr, qi - pi)
        vi = jnp.where(first, qi, pr - qr)
        sides.append((jnp.concatenate([ur, vr], axis=1), jnp.concatenate([ui, vi], axis=1)))
    (pr, pi), (qr, qi) = sides
    ur = rows_fixed(pr, pr + qr)
    ui = rows_fixed(pi, pi + qi)
    vr = rows_fixed(qr, qi - pi)
    vi = rows_fixed(qi, pr - qr)
    return jnp.concatenate([ur, vr, ui, vi], axis=0)


def read_plane(ref, plane):
    if plane == 3:
        value = ref[pl.ds(2 * CHUNKS, CHUNKS), pl.ds(0, 16), :]
        return value.reshape(R, R)
    start, stop = plane * R, (plane + 1) * R
    low, high = start // ROWS, -(-stop // ROWS)
    value = ref[pl.ds(low, high - low)].reshape((high - low) * ROWS, R)
    return value[start - low * ROWS : stop - low * ROWS]


def write_plane(ref, plane, value):
    if plane == 3:
        for chunk in range(CHUNKS):
            ref[2 * CHUNKS + chunk, pl.ds(0, 16), :] = value[16 * chunk : 16 * chunk + 16]
        return
    for tile in range(R // 8):
        row = plane * R + 8 * tile
        ref[row // ROWS, pl.ds(row % ROWS, 8), :] = value[8 * tile : 8 * tile + 8]


def whole_kernel(
    offs, cnt, obj_in, probe_in, patterns_in, tabs_in,
    obj_out, probe_out,
    obj, probe, tabs, pad, pbuf, gbuf, spat, patch, far, og, zbuf, grad, cover,
    acc0, acc1, recv0, recv1, recv2, cross, hside, hvert, hcorn,
    load, bsend, brecv, hsend, hrecv, gsend, grecv,
):
    wide = lax.axis_index("wide")
    x = lax.axis_index("narrow")
    n_wide = lax.axis_size("wide")
    n_narrow = lax.axis_size("narrow")
    core = wide % 2
    z = (wide // 2) % 4
    y = wide // 8
    place = (x, y, z)
    table = (tabs.at[0], tabs.at[1])
    table_t = (tabs.at[2], tabs.at[3])

    def device(at, c):
        return ((at[1] * 4 + at[2]) * 2 + c, at[0])

    def peer(dim, step):
        at = list(place)
        at[dim] = (at[dim] + step) % 4
        return device(at, core)

    sibling = device(place, 1 - core)

    left, right, above, below = ways = ((-1, 0), (1, 0), (0, -1), (0, 1))

    def there(way):
        if way[0]:
            return (wide > 0) if way[0] < 0 else (wide < n_wide - 1)
        return (x > 0) if way[1] < 0 else (x < n_narrow - 1)

    def away(way):
        return (wide + way[0], x + way[1])

    def back(way):
        return (-way[0], -way[1])

    loads = [
        pltpu.make_async_copy(source, target, load.at[index])
        for index, (source, target) in enumerate(
            ((obj_in, obj), (tabs_in, tabs), (patterns_in, spat), (probe_in, probe))
        )
    ]
    for one in loads:
        one.start()

    barrier = pltpu.get_barrier_semaphore()
    pl.semaphore_signal(barrier, inc=1, device_id=sibling, device_id_type=MESH)
    for dim in range(3):
        for step in STEPS:
            pl.semaphore_signal(barrier, inc=1, device_id=peer(dim, step), device_id_type=MESH)
    total = 10
    for way in ways:
        total = total + there(way).astype(jnp.int32)

        @pl.when(there(way))
        def _():
            pl.semaphore_signal(barrier, inc=1, device_id=away(way), device_id_type=MESH)

    pl.semaphore_wait(barrier, total)
    loads[0].wait()

    def neighbour_copy(source, target, send_sem, recv_sem, index, way):
        return pltpu.make_async_remote_copy(
            src_ref=source,
            dst_ref=target,
            send_sem=send_sem.at[index],
            recv_sem=recv_sem.at[index],
            device_id=away(way),
            device_id_type=MESH,
        )

    def halo(index):
        if index < 2:
            way = ways[index]
            lane_from, lane_to = ((0, 5), (3, 0))[index]
            source = obj.at[:, :, pl.ds(lane_from * H, H)]
            return way, True, neighbour_copy(
                source, pad.at[:, lane_to, pl.ds(H, TILE), :], hsend, hrecv, index, way
            )
        if index < 10:
            lane = (0, 3, 1, 2)[(index - 2) // 2]
            side = (index - 2) % 2
            row_from, row_to = ((0, H + TILE), (TILE - H, 0))[side]
            source = obj.at[:, pl.ds(row_from, H), pl.ds(lane * H, H)]
            return ways[2 + side], True, neighbour_copy(
                source, pad.at[:, lane + 1, pl.ds(row_to, H), :], hsend, hrecv, index, ways[2 + side]
            )
        vertical, side = divmod(index - 10, 2)
        lane_from, lane_to = ((1, 5), (4, 0))[side]
        rows = pl.ds(vertical * (H + TILE), H)
        return ways[side], there(ways[2 + vertical]), neighbour_copy(
            pad.at[:, lane_from, rows, :], pad.at[:, lane_to, rows, :], hsend, hrecv, index, ways[side]
        )

    def both_there(way, also):
        return there(way) if also is True else jnp.logical_and(there(way), also)

    def start_if(copy):
        way, also, one = copy

        @pl.when(both_there(way, also))
        def _():
            one.start()

    def wait_send_if(copy):
        way, also, one = copy

        @pl.when(both_there(way, also))
        def _():
            one.wait_send()

    def wait_recv_if(copy):
        way, also, one = copy

        @pl.when(both_there(back(way), also))
        def _():
            one.wait_recv()

    for index in range(2, 10):
        start_if(halo(index))
    for index in range(2):
        start_if(halo(index))

    for side in range(2):
        lane = (0, 5)[side]

        @pl.when(jnp.logical_not(there(ways[side])))
        def _():
            for at in range(2):
                pad[at, lane, pl.ds(H, TILE), :] = jnp.zeros((TILE, H), F32)
            hside[1 - side] = jnp.zeros((2, TILE, H), F32)

        for vertical in range(2):

            @pl.when(jnp.logical_not(jnp.logical_and(there(ways[side]), there(ways[2 + vertical]))))
            def _():
                for at in range(2):
                    pad[at, lane, pl.ds(vertical * (H + TILE), H), :] = jnp.zeros((H, H), F32)

    for vertical in range(2):

        @pl.when(jnp.logical_not(there(ways[2 + vertical])))
        def _():
            for at in range(2):
                for lane in range(1, 5):
                    pad[at, lane, pl.ds(vertical * (H + TILE), H), :] = jnp.zeros((H, H), F32)
            hvert[1 - vertical] = jnp.zeros((2, 4, H, H), F32)

    for at in range(2):
        for lane in range(4):
            pad[at, lane + 1, pl.ds(H, TILE), :] = obj[at, :, pl.ds(lane * H, H)]
    for one in loads[1:]:
        one.wait()
    for half in range(2):
        for plane in range(4):
            write_plane(pbuf.at[0, half], plane, probe[half * 2 + plane // 2, plane % 2])
        for chunk in range(CHUNKS):
            pbuf[0, half, 2 * CHUNKS + chunk, pl.ds(16, 8), :] = jnp.zeros((8, R), F32)
    zbuf[...] = jnp.zeros_like(zbuf)
    grad[...] = jnp.zeros_like(grad)

    @pl.loop(0, BATCHES * POS)
    def _(slot):
        high, low = split(jnp.sqrt(spat[slot]))
        high, low = split(dot(tabs[4], high) + dot(tabs[4], low))
        spat[slot] = dot(high, tabs[5]) + dot(low, tabs[5])

    for index in range(2, 6):
        wait_recv_if(halo(index))
    for index in range(10, 14):
        start_if(halo(index))
    for index in (0, 1, 6, 7, 8, 9, 10, 11, 12, 13):
        wait_recv_if(halo(index))
    for index in range(14):
        wait_send_if(halo(index))

    lanes = lax.broadcasted_iota(jnp.int32, (R, H), 1)

    def window(slot):
        row = offs[0, slot] + H
        col = offs[1, slot] + H
        first = jnp.minimum(col // H, 3)
        return row, first, col - first * H

    def take_patches(batch):
        covered = jnp.zeros((8, R), F32)
        for position in range(POS):
            slot = batch * POS + position
            row, first, shift = window(slot)
            live = slot < cnt[0]
            turn = (H - shift) % H
            for at in range(2):
                turned = [
                    pltpu.roll(pad[at, first + k, pl.ds(row, R), :], turn, 1) for k in range(3)
                ]
                for k in range(2):
                    value = jnp.where(lanes < H - shift, turned[k], turned[k + 1])
                    value = jnp.where(live, value, 0.0)
                    patch[position, at, :, pl.ds(k * H, H)] = value
                    covered = covered + jnp.sum(value * value)
        cover[...] = covered

    take_patches(0)

    def half_planes(ref, mode):
        return read_plane(ref, 2 * mode), read_plane(ref, 2 * mode + 1)

    def run_batch(batch):
        for half in range(2):
            for chunk in range(CHUNKS):
                gbuf[half, 2 * CHUNKS + chunk, pl.ds(16, 8), :] = cover[...]

        @pl.loop(0, 2)
        def _(turn):
            half = (core + turn) % 2

            @pl.when(jnp.logical_and(turn == 1, batch > 0))
            def _():
                all_reduce_end(batch - 1)

            for mode in range(2):
                pr, pi = half_planes(pbuf.at[batch, half], mode)
                for position in range(POS):
                    our, oui = patch[position, 0], patch[position, 1]
                    psi = jnp.concatenate([pr * our - pi * oui, pr * oui + pi * our], axis=1)
                    left = left_product((table[0][...], table[1][...]), psi)
                    left = jnp.concatenate([left[:, :R], left[:, R:]], axis=0)
                    both = right_product(left, (table_t[0][...], table_t[1][...]))
                    quads = butterfly(both[:R], both[R:])
                    slot = half * 2 + mode
                    for a in range(2):
                        for b in range(2):
                            for at in range(2):
                                far[position, slot, at, pl.ds(a * HALF, HALF), pl.ds(b * HALF, HALF)] = (
                                    quads[a][b][at]
                                )

        for position in range(POS):
            for tile in range(R // 32):
                rows = pl.ds(tile * 32, 32)
                power = jnp.zeros((32, R), F32)
                for mode in range(MODES):
                    re, im = far[position, mode, 0, rows, :], far[position, mode, 1, rows, :]
                    power = power + re * re + im * im
                slot = batch * POS + position
                spat[slot, rows, :] = 1.0 - spat[slot, rows, :] * lax.rsqrt(power + 0.1)

        for turn in range(2):
            half = (core + 1 + turn) % 2
            for mode in range(2):
                pr, pi = half_planes(pbuf.at[batch, half], mode)
                sum_re, sum_im = None, None
                for position in range(POS):
                    slot = half * 2 + mode
                    quads = []
                    for a in range(2):
                        row = []
                        for b in range(2):
                            rows, cols = pl.ds(a * HALF, HALF), pl.ds(b * HALF, HALF)
                            keep = spat[batch * POS + position, rows, cols]
                            row.append(
                                (
                                    far[position, slot, 0, rows, cols] * keep,
                                    far[position, slot, 1, rows, cols] * keep,
                                )
                            )
                        quads.append(row)
                    both = butterfly_transposed(quads)
                    right = right_product(both, (table[0][...], table[1][...]))
                    right = jnp.concatenate([right[:R], right[R:]], axis=1)
                    back = left_product((table_t[0][...], table_t[1][...]), right)
                    dr, di = back[:, :R], back[:, R:]
                    our, oui = patch[position, 0], patch[position, 1]
                    og_re = pr * dr + pi * di
                    og_im = pr * di - pi * dr
                    if turn == 0 and mode == 0:
                        og[position, 0] = og_re
                        og[position, 1] = og_im
                    else:
                        og[position, 0] += og_re
                        og[position, 1] += og_im
                    pg_re = our * dr + oui * di
                    pg_im = our * di - oui * dr
                    sum_re = pg_re if sum_re is None else sum_re + pg_re
                    sum_im = pg_im if sum_im is None else sum_im + pg_im
                write_plane(gbuf.at[half], 2 * mode, sum_re)
                write_plane(gbuf.at[half], 2 * mode + 1, sum_im)
            if turn == 0:
                for part in range(PARTS):
                    to_sibling(batch, part).start()

    def add_gradient(batch):
        rows, firsts = [], []
        for position in range(POS):
            row, first, shift = window(batch * POS + position)
            rows.append(row)
            firsts.append(first)
            turn = shift % H
            for at in range(2):
                low = pltpu.roll(og[position, at, :, pl.ds(0, H)], turn, 1)
                high = pltpu.roll(og[position, at, :, pl.ds(H, H)], turn, 1)
                zbuf[position, at, 1, pl.ds(8, R), :] = jnp.where(lanes >= shift, low, 0.0)
                zbuf[position, at, 2, pl.ds(8, R), :] = jnp.where(lanes >= shift, high, low)
                zbuf[position, at, 3, pl.ds(8, R), :] = jnp.where(lanes >= shift, 0.0, high)

        def add_rows(base, which):
            for sub in range(2):
                at_row = pl.multiple_of(base + 8 * sub, 8)
                starts = [jnp.clip(at_row - row + 8, 0, R + 8) for row in rows]
                for at in range(2):
                    for lane in which:
                        value = grad[at, lane, pl.ds(at_row, 8), :]
                        for position in range(POS):
                            source = jnp.clip(lane - firsts[position] + 1, 0, 4)
                            value = value + zbuf[position, at, source, pl.ds(starts[position], 8), :]
                        grad[at, lane, pl.ds(at_row, 8), :] = value

        @pl.loop(0, 2 * H // 16)
        def _(tile):
            add_rows(tile * 16 + (tile // (H // 16)) * TILE, range(6))

        @pl.loop(0, TILE // 16)
        def _(tile):
            add_rows(H + tile * 16, (0, 5))

        border_turn(batch, 0)

        @pl.loop(0, TILE // 16)
        def _(tile):
            add_rows(H + tile * 16, range(1, 5))

    def border_copy(index):
        if index < 4:
            vertical, side = divmod(index, 2)
            rows = pl.ds(vertical * (H + TILE), H)
            return ways[side], True, neighbour_copy(
                grad.at[:, (0, 5)[side], rows, :], hcorn.at[vertical, side], gsend, grecv, index, ways[side]
            )
        if index < 12:
            piece, side = divmod(index - 4, 2)
            return ways[side], True, neighbour_copy(
                grad.at[:, (0, 5)[side], pl.ds(H + H * piece, H), :],
                hside.at[side, :, pl.ds(H * piece, H), :],
                gsend, grecv, index, ways[side],
            )
        lane = (1, 2, 0, 3)[(index - 12) // 2]
        vertical = (index - 12) % 2
        rows = pl.ds(vertical * (H + TILE), H)
        return ways[2 + vertical], True, neighbour_copy(
            grad.at[:, lane + 1, rows, :], hvert.at[vertical, :, lane], gsend, grecv, index, ways[2 + vertical]
        )

    def pass_corners():
        for index in range(4):
            vertical, side = divmod(index, 2)
            rows = pl.ds(vertical * (H + TILE), H)
            lane = (4, 1)[side]
            way, _, one = border_copy(index)

            @pl.when(there(back(way)))
            def _():
                one.wait_recv()
                for at in range(2):
                    grad[at, lane, rows, :] += hcorn[vertical, side, at]

    def border_turn(batch, turn):
        @pl.when(batch == BATCHES - 1)
        def _():
            if turn == 0:
                for index in range(4):
                    start_if(border_copy(index))
            if turn == 2:
                pass_corners()
            for index in (2 * turn + 12, 2 * turn + 13, 2 * turn + 4, 2 * turn + 5):
                start_if(border_copy(index))

    def to_sibling(batch, part):
        span = pl.ds(part * CHUNKS, CHUNKS)
        return pltpu.make_async_remote_copy(
            src_ref=gbuf.at[1 - core, span],
            dst_ref=recv0.at[batch, span],
            send_sem=bsend.at[part],
            recv_sem=brecv.at[batch, part],
            device_id=sibling,
            device_id_type=MESH,
        )

    def shared(batch, part, step):
        chunk = part * CHUNKS + 4 * ((place[ORDER[part][0]] + 4 - step) % 4)
        group = pl.ds(chunk, 4)
        index = part * 4 + step

        def copy(half):
            ref = pbuf.at[batch + 1, half, group, pl.ds(0, KEPT[part])]
            return pltpu.make_async_remote_copy(
                src_ref=ref,
                dst_ref=ref,
                send_sem=bsend.at[3 + index],
                recv_sem=brecv.at[batch, 3 + index],
                device_id=sibling,
                device_id_type=MESH,
            )

        return copy

    def all_reduce_end(batch):
        for step in range(4):
            for part in range(PARTS):
                shared(batch, part, step)(1 - core).wait_recv()
                shared(batch, part, step)(core).wait_send()

    def gather_sent(batch):
        for index in range(45):
            part = (index // 3) % 3
            ref = pbuf.at[batch + 1, core, part, pl.ds(0, KEPT[part])]
            pltpu.make_async_remote_copy(
                src_ref=ref,
                dst_ref=ref,
                send_sem=bsend.at[15 + 54 + index],
                recv_sem=brecv.at[batch, 0],
                device_id=sibling,
                device_id_type=MESH,
            ).wait_send()

    def all_reduce(batch):
        new = pbuf.at[batch + 1]
        old = pbuf.at[batch]

        def copy(source, target, index, to, send=0):
            return pltpu.make_async_remote_copy(
                src_ref=source,
                dst_ref=target,
                send_sem=bsend.at[send],
                recv_sem=brecv.at[batch, index],
                device_id=to,
                device_id_type=MESH,
            )

        sent = []

        def send(source, target, index, to):
            one = copy(source, target, index, to, 15 + len(sent))
            one.start()
            sent.append(one)

        def first_at(part, order):
            return (place[ORDER[part][1]] + 1 + order) % 4

        for part in range(PARTS):
            span = pl.ds(part * CHUNKS, CHUNKS)
            d1 = ORDER[part][0]
            to_sibling(batch, part).wait_recv()
            to_sibling(batch, part).wait_send()
            acc0[span] = gbuf[core, span] + recv0[batch, span]
            for order in range(4):
                for step in STEPS:
                    chunk = part * CHUNKS + 4 * ((place[d1] + step) % 4) + first_at(part, order)
                    target = recv1.at[batch, part, order, step - 1]
                    send(acc0.at[chunk], target, 15 + part * 4 + order, peer(d1, step))

        add_gradient(batch)

        @pl.when(batch > 0)
        def _():
            gather_sent(batch - 1)

        lasts = []
        for order in range(4):
            for part in range(PARTS):
                d1, d2, _ = ORDER[part]
                quarter = recv1.at[batch, part, order]
                copy(acc0.at[pl.ds(0, 3)], quarter, 15 + part * 4 + order, peer(d1, 1)).wait_recv()
                value = acc0[part * CHUNKS + 4 * place[d1] + first_at(part, order)]
                for step in STEPS:
                    value = value + quarter[step - 1]
                if order == 3:
                    lasts.append(value)
                else:
                    acc1[part, order] = value
                    target = recv2.at[batch, part, order]
                    send(acc1.at[part, order], target, 27 + part, peer(d2, order + 1))

        for part in range(PARTS):
            acc1[part, 3] = lasts[part]
        border_turn(batch, 1)

        @pl.when(batch < BATCHES - 1)
        def _():
            take_patches(batch + 1)

        for part in range(PARTS):
            _, d2, d3 = ORDER[part]
            copy(acc1.at[part, pl.ds(0, 3)], recv2.at[batch, part], 27 + part, peer(d2, 1)).wait_recv()
            value = acc1[part, 3]
            for step in STEPS:
                value = value + recv2[batch, part, step - 1]
            cross[batch, part, place[d3]] = value
            for step in STEPS:
                mine = cross.at[batch, part, place[d3]]
                send(mine, mine, 30 + part * 3 + step - 1, peer(d3, step))

        border_turn(batch, 2)
        for one in sent[:45]:
            one.wait_send()
        sums = []
        for part in range(PARTS):
            d3 = ORDER[part][2]
            for step in STEPS:
                theirs = cross.at[batch, part, (place[d3] + 4 - step) % 4]
                copy(theirs, theirs, 30 + part * 3 + step - 1, peer(d3, step)).wait_recv()
            value = cross[batch, part, 0]
            for at in range(1, 4):
                value = value + cross[batch, part, at]
            sums.append(value)
        scale = sums[2][16:] / float(R * R)
        scale = jnp.concatenate([scale, scale, scale], axis=0)

        def gather(part, chunk):
            d1 = ORDER[part][0]
            ref = new.at[core, chunk, pl.ds(0, KEPT[part])]
            for step in STEPS:
                send(ref, ref, 48 + part * 3 + step - 1, peer(d1, step))

        chunks = []
        for part in range(PARTS):
            d1, d2, _ = ORDER[part]
            chunk = part * CHUNKS + 4 * place[d1] + place[d2]
            chunks.append(chunk)
            new[core, chunk] = old[core, chunk] - sums[part] / scale
            for step in STEPS:
                mine = new.at[core, chunk, pl.ds(0, KEPT[part])]
                send(mine, mine, 39 + part * 3 + step - 1, peer(d2, step))
        for part in range(PARTS):
            gather(part, chunks[part])
        border_turn(batch, 3)
        for step in (1, 3, 2):
            for part in range(PARTS):
                d1, d2, _ = ORDER[part]
                chunk = part * CHUNKS + 4 * place[d1] + (place[d2] + 4 - step) % 4
                theirs = new.at[core, chunk, pl.ds(0, KEPT[part])]
                copy(theirs, theirs, 39 + part * 3 + step - 1, peer(d2, step)).wait_recv()
                gather(part, chunk)
        for part in range(PARTS):
            shared(batch, part, 0)(core).start()
        for step in (1, 3, 2):
            for part in range(PARTS):
                d1 = ORDER[part][0]
                group = new.at[
                    core, pl.ds(part * CHUNKS + 4 * ((place[d1] + 4 - step) % 4), 4), pl.ds(0, KEPT[part])
                ]
                copy(group, group, 48 + part * 3 + step - 1, peer(d1, step)).wait_recv()
                shared(batch, part, step)(core).start()
        for one in sent[45:54]:
            one.wait_send()

    @pl.loop(0, BATCHES)
    def _(batch):
        run_batch(batch)
        all_reduce(batch)

    gather_sent(BATCHES - 1)
    all_reduce_end(BATCHES - 1)

    power = jnp.zeros((R, R), F32)
    for half in range(2):
        for plane in range(4):
            value = read_plane(pbuf.at[BATCHES, half], plane)
            probe_out[half * 2 + plane // 2, plane % 2] = value
            power = power + value * value
    part_of_top = 0.5 / jnp.max(power)

    for index in range(4, 20):
        wait_recv_if(border_copy(index))
    for index in range(20):
        wait_send_if(border_copy(index))

    def came(lane, row, rows, at):
        value = grad[at, lane + 1, pl.ds(H + row, rows), :]
        if lane == 0:
            value = value + hside[1, at, pl.ds(row, rows), :]
        if lane == 3:
            value = value + hside[0, at, pl.ds(row, rows), :]
        if row == 0:
            value = value + hvert[1, at, lane]
        if row == TILE - H:
            value = value + hvert[0, at, lane]
        return value

    for at in range(2):
        for lane in range(4):
            for row in range(0, TILE, H):
                place_at = (at, pl.ds(row, H), pl.ds(lane * H, H))
                obj_out[place_at] = obj[place_at] - came(lane, row, H, at) * part_of_top


def ship_kernel(obj, probe, obj_out, probe_out, sems):
    copies = [
        pltpu.make_async_copy(obj, obj_out, sems.at[0]),
        pltpu.make_async_copy(probe, probe_out, sems.at[1]),
    ]
    for one in copies:
        one.start()
    for one in copies:
        one.wait()


def local(object_field, probe, patterns, offsets, counts):
    vmem = pl.BlockSpec(memory_space=pltpu.VMEM)
    hbm = pl.BlockSpec(memory_space=pltpu.HBM)
    smem = pl.BlockSpec(memory_space=pltpu.SMEM)
    dma = pltpu.SemaphoreType.DMA
    done = pl.pallas_call(
        whole_kernel,
        out_shape=(
            pltpu.VMEM((2, TILE, TILE), F32),
            pltpu.VMEM((MODES, 2, R, R), F32),
        ),
        in_specs=[smem, smem, hbm, hbm, hbm, hbm],
        out_specs=(vmem, vmem),
        scratch_shapes=[
            pltpu.VMEM((2, TILE, TILE), F32),
            pltpu.VMEM((MODES, 2, R, R), F32),
            pltpu.VMEM((6, R, R), BF16),
            pltpu.VMEM((2, 6, TILE + 2 * H, H), F32),
            pltpu.VMEM((BATCHES + 1, 2, PARTS * CHUNKS, ROWS, R), F32),
            pltpu.VMEM((2, PARTS * CHUNKS, ROWS, R), F32),
            pltpu.VMEM((BATCHES * POS, R, R), F32),
            pltpu.VMEM((POS, 2, R, R), F32),
            pltpu.VMEM((POS, MODES, 2, R, R), F32),
            pltpu.VMEM((POS, 2, R, R), F32),
            pltpu.VMEM((POS, 2, 5, R + 16, H), F32),
            pltpu.VMEM((2, 6, TILE + 2 * H, H), F32),
            pltpu.VMEM((8, R), F32),
            pltpu.VMEM((PARTS * CHUNKS, ROWS, R), F32),
            pltpu.VMEM((PARTS, 4, ROWS, R), F32),
            pltpu.VMEM((BATCHES, PARTS * CHUNKS, ROWS, R), F32),
            pltpu.VMEM((BATCHES, PARTS, 4, 3, ROWS, R), F32),
            pltpu.VMEM((BATCHES, PARTS, 3, ROWS, R), F32),
            pltpu.VMEM((BATCHES, PARTS, 4, ROWS, R), F32),
            pltpu.VMEM((2, 2, TILE, H), F32),
            pltpu.VMEM((2, 2, 4, H, H), F32),
            pltpu.VMEM((2, 2, 2, H, H), F32),
            dma((4,)),
            dma((114,)),
            dma((BATCHES, 57)),
            dma((14,)),
            dma((14,)),
            dma((20,)),
            dma((20,)),
        ],
        compiler_params=pltpu.CompilerParams(
            collective_id=0, has_side_effects=True, vmem_limit_bytes=56 * 1024 * 1024
        ),
    )(
        offsets.reshape(BATCHES * POS, 2).T,
        counts.reshape(1),
        object_field,
        probe,
        patterns.reshape(BATCHES * POS, R, R),
        jnp.asarray(tables()),
    )
    return pl.pallas_call(
        ship_kernel,
        out_shape=(
            jax.ShapeDtypeStruct((2, TILE, TILE), F32),
            jax.ShapeDtypeStruct((MODES, 2, R, R), F32),
        ),
        in_specs=[vmem, vmem],
        out_specs=(hbm, hbm),
        scratch_shapes=[dma((2,))],
        compiler_params=pltpu.CompilerParams(vmem_limit_bytes=1024 * 1024),
    )(*done)


def solution(mesh):
    placed = (
        P(None, "narrow", "wide"),
        P(),
        P("narrow", "wide", None, None, None),
        P("narrow", "wide", None, None),
        P("narrow", "wide"),
    )
    return jax.shard_map(
        local,
        mesh=mesh,
        in_specs=placed,
        out_specs=(P(None, "narrow", "wide"), P()),
        check_vma=False,
    )
```

```python
import jax
import jax.numpy as jnp
import ml_dtypes
import numpy as np
from jax import lax
from jax.experimental import pallas as pl
from jax.experimental.pallas import tpu as pltpu
from jax.sharding import PartitionSpec as P

H = 128
TILE = 512
R = 256
HALF = R // 2
MODES = 4
BATCHES = 3
POS = 2
MESH = pl.DeviceIdType.MESH
F32 = jnp.float32
BF16 = jnp.bfloat16

PARTS = 3
CHUNKS = 16
ROWS = 24
ORDER = ((1, 2, 0), (2, 0, 1), (0, 1, 2))
KEPT = (24, 24, 16)
STEPS = (2, 1, 3)


def tables():
    k = np.arange(R)
    angle = 2.0 * np.pi * ((np.arange(HALF)[:, None] * k[None, :]) % R) / R
    upper = np.cos(angle)
    lower = np.sin(angle)
    lower[0] = np.where(k % 2 == 0, 1.0, -1.0)
    packed = (np.concatenate([upper, lower]) / np.sqrt(R)).astype(np.float32)
    order = np.concatenate([np.arange(HALF), [HALF], R - np.arange(1, HALF)])
    select = np.zeros((R, R), np.float32)
    select[np.arange(R), order] = 1.0

    def pair(value):
        high = value.astype(ml_dtypes.bfloat16)
        low = (value - high.astype(np.float32)).astype(ml_dtypes.bfloat16)
        return [high, low]

    pick = select.astype(ml_dtypes.bfloat16)
    return np.stack(pair(packed) + pair(packed.T.copy()) + [pick, pick.T.copy()])


def split(value):
    high = value.astype(BF16)
    return high, (value - high.astype(F32)).astype(BF16)


def dot(a, b):
    return jnp.dot(a, b, preferred_element_type=F32)


def left_product(table, value):
    high, low = split(value)
    return dot(table[0], high) + dot(table[0], low) + dot(table[1], high)


def right_product(value, table):
    high, low = split(value)
    return dot(high, table[0]) + dot(low, table[0]) + dot(high, table[1])


def row_mask(shape):
    return lax.broadcasted_iota(jnp.int32, shape, 0) == 0


def rows_fixed(first, general):
    top = jnp.where(row_mask(first[:8].shape), first[:8], general[:8])
    return jnp.concatenate([top, general[8:]], axis=0)


def butterfly(zr, zi):
    ur, vr, ui, vi = zr[:HALF], zr[HALF:], zi[:HALF], zi[HALF:]
    plus = (rows_fixed(ur, ur + vi), rows_fixed(ui, ui - vr))
    minus = (rows_fixed(vr, ur - vi), rows_fixed(vi, ui + vr))
    first = lax.broadcasted_iota(jnp.int32, (HALF, HALF), 1) == 0
    out = []
    for re, im in (plus, minus):
        ur, vr, ui, vi = re[:, :HALF], re[:, HALF:], im[:, :HALF], im[:, HALF:]
        mr, mi = jnp.where(first, 0.0, vr), jnp.where(first, 0.0, vi)
        out.append(
            (
                (ur + mi, ui - mr),
                (jnp.where(first, vr, ur - vi), jnp.where(first, vi, ui + vr)),
            )
        )
    return out


def butterfly_transposed(quads):
    first = lax.broadcasted_iota(jnp.int32, (HALF, HALF), 1) == 0
    sides = []
    for (pr, pi), (qr, qi) in quads:
        ur = pr + jnp.where(first, 0.0, qr)
        ui = pi + jnp.where(first, 0.0, qi)
        vr = jnp.where(first, qr, qi - pi)
        vi = jnp.where(first, qi, pr - qr)
        sides.append((jnp.concatenate([ur, vr], axis=1), jnp.concatenate([ui, vi], axis=1)))
    (pr, pi), (qr, qi) = sides
    ur = rows_fixed(pr, pr + qr)
    ui = rows_fixed(pi, pi + qi)
    vr = rows_fixed(qr, qi - pi)
    vi = rows_fixed(qi, pr - qr)
    return jnp.concatenate([ur, vr, ui, vi], axis=0)


def read_plane(ref, plane):
    if plane == 3:
        value = ref[pl.ds(2 * CHUNKS, CHUNKS), pl.ds(0, 16), :]
        return value.reshape(R, R)
    start, stop = plane * R, (plane + 1) * R
    low, high = start // ROWS, -(-stop // ROWS)
    value = ref[pl.ds(low, high - low)].reshape((high - low) * ROWS, R)
    return value[start - low * ROWS : stop - low * ROWS]


def write_plane(ref, plane, value):
    if plane == 3:
        for chunk in range(CHUNKS):
            ref[2 * CHUNKS + chunk, pl.ds(0, 16), :] = value[16 * chunk : 16 * chunk + 16]
        return
    for tile in range(R // 8):
        row = plane * R + 8 * tile
        ref[row // ROWS, pl.ds(row % ROWS, 8), :] = value[8 * tile : 8 * tile + 8]


def whole_kernel(
    offs, cnt, obj_in, probe_in, patterns_in, tabs_in,
    obj_out, probe_out,
    obj, probe, tabs, pad, pbuf, gbuf, spat, patch, far, og, zbuf, grad, cover,
    acc0, acc1, recv0, recv1, recv2, cross, hside, hvert, hcorn,
    load, bsend, brecv, hsend, hrecv, gsend, grecv,
):
    wide = lax.axis_index("wide")
    x = lax.axis_index("narrow")
    n_wide = lax.axis_size("wide")
    n_narrow = lax.axis_size("narrow")
    core = wide % 2
    z = (wide // 2) % 4
    y = wide // 8
    place = (x, y, z)
    table = (tabs.at[0], tabs.at[1])
    table_t = (tabs.at[2], tabs.at[3])

    def device(at, c):
        return ((at[1] * 4 + at[2]) * 2 + c, at[0])

    def peer(dim, step):
        at = list(place)
        at[dim] = (at[dim] + step) % 4
        return device(at, core)

    sibling = device(place, 1 - core)

    left, right, above, below = ways = ((-1, 0), (1, 0), (0, -1), (0, 1))

    def there(way):
        if way[0]:
            return (wide > 0) if way[0] < 0 else (wide < n_wide - 1)
        return (x > 0) if way[1] < 0 else (x < n_narrow - 1)

    def away(way):
        return (wide + way[0], x + way[1])

    def back(way):
        return (-way[0], -way[1])

    loads = [
        pltpu.make_async_copy(source, target, load.at[index])
        for index, (source, target) in enumerate(
            ((obj_in, obj), (tabs_in, tabs), (patterns_in, spat), (probe_in, probe))
        )
    ]
    for one in loads:
        one.start()

    barrier = pltpu.get_barrier_semaphore()
    pl.semaphore_signal(barrier, inc=1, device_id=sibling, device_id_type=MESH)
    for dim in range(3):
        for step in STEPS:
            pl.semaphore_signal(barrier, inc=1, device_id=peer(dim, step), device_id_type=MESH)
    total = 10
    for way in ways:
        total = total + there(way).astype(jnp.int32)

        @pl.when(there(way))
        def _():
            pl.semaphore_signal(barrier, inc=1, device_id=away(way), device_id_type=MESH)

    pl.semaphore_wait(barrier, total)
    loads[0].wait()

    def neighbour_copy(source, target, send_sem, recv_sem, index, way):
        return pltpu.make_async_remote_copy(
            src_ref=source,
            dst_ref=target,
            send_sem=send_sem.at[index],
            recv_sem=recv_sem.at[index],
            device_id=away(way),
            device_id_type=MESH,
        )

    def halo(index):
        if index < 2:
            way = ways[index]
            lane_from, lane_to = ((0, 5), (3, 0))[index]
            source = obj.at[:, :, pl.ds(lane_from * H, H)]
            return way, True, neighbour_copy(
                source, pad.at[:, lane_to, pl.ds(H, TILE), :], hsend, hrecv, index, way
            )
        if index < 10:
            lane = (0, 3, 1, 2)[(index - 2) // 2]
            side = (index - 2) % 2
            row_from, row_to = ((0, H + TILE), (TILE - H, 0))[side]
            source = obj.at[:, pl.ds(row_from, H), pl.ds(lane * H, H)]
            return ways[2 + side], True, neighbour_copy(
                source, pad.at[:, lane + 1, pl.ds(row_to, H), :], hsend, hrecv, index, ways[2 + side]
            )
        vertical, side = divmod(index - 10, 2)
        lane_from, lane_to = ((1, 5), (4, 0))[side]
        rows = pl.ds(vertical * (H + TILE), H)
        return ways[side], there(ways[2 + vertical]), neighbour_copy(
            pad.at[:, lane_from, rows, :], pad.at[:, lane_to, rows, :], hsend, hrecv, index, ways[side]
        )

    def both_there(way, also):
        return there(way) if also is True else jnp.logical_and(there(way), also)

    def start_if(copy):
        way, also, one = copy

        @pl.when(both_there(way, also))
        def _():
            one.start()

    def wait_send_if(copy):
        way, also, one = copy

        @pl.when(both_there(way, also))
        def _():
            one.wait_send()

    def wait_recv_if(copy):
        way, also, one = copy

        @pl.when(both_there(back(way), also))
        def _():
            one.wait_recv()

    for index in range(2, 10):
        start_if(halo(index))
    for index in range(2):
        start_if(halo(index))

    for side in range(2):
        lane = (0, 5)[side]

        @pl.when(jnp.logical_not(there(ways[side])))
        def _():
            for at in range(2):
                pad[at, lane, pl.ds(H, TILE), :] = jnp.zeros((TILE, H), F32)
            hside[1 - side] = jnp.zeros((2, TILE, H), F32)

        for vertical in range(2):

            @pl.when(jnp.logical_not(jnp.logical_and(there(ways[side]), there(ways[2 + vertical]))))
            def _():
                for at in range(2):
                    pad[at, lane, pl.ds(vertical * (H + TILE), H), :] = jnp.zeros((H, H), F32)

    for vertical in range(2):

        @pl.when(jnp.logical_not(there(ways[2 + vertical])))
        def _():
            for at in range(2):
                for lane in range(1, 5):
                    pad[at, lane, pl.ds(vertical * (H + TILE), H), :] = jnp.zeros((H, H), F32)
            hvert[1 - vertical] = jnp.zeros((2, 4, H, H), F32)

    for at in range(2):
        for lane in range(4):
            pad[at, lane + 1, pl.ds(H, TILE), :] = obj[at, :, pl.ds(lane * H, H)]
    for one in loads[1:]:
        one.wait()
    for half in range(2):
        for plane in range(4):
            write_plane(pbuf.at[0, half], plane, probe[half * 2 + plane // 2, plane % 2])
        for chunk in range(CHUNKS):
            pbuf[0, half, 2 * CHUNKS + chunk, pl.ds(16, 8), :] = jnp.zeros((8, R), F32)
    zbuf[...] = jnp.zeros_like(zbuf)
    grad[...] = jnp.zeros_like(grad)

    @pl.loop(0, BATCHES * POS)
    def _(slot):
        high, low = split(jnp.sqrt(spat[slot]))
        high, low = split(dot(tabs[4], high) + dot(tabs[4], low))
        spat[slot] = dot(high, tabs[5]) + dot(low, tabs[5])

    for index in range(2, 6):
        wait_recv_if(halo(index))
    for index in range(10, 14):
        start_if(halo(index))
    for index in (0, 1, 6, 7, 8, 9, 10, 11, 12, 13):
        wait_recv_if(halo(index))
    for index in range(14):
        wait_send_if(halo(index))

    lanes = lax.broadcasted_iota(jnp.int32, (R, H), 1)

    def window(slot):
        row = offs[0, slot] + H
        col = offs[1, slot] + H
        first = jnp.minimum(col // H, 3)
        return row, first, col - first * H

    def take_patches(batch):
        covered = jnp.zeros((8, R), F32)
        for position in range(POS):
            slot = batch * POS + position
            row, first, shift = window(slot)
            live = slot < cnt[0]
            turn = (H - shift) % H
            for at in range(2):
                turned = [
                    pltpu.roll(pad[at, first + k, pl.ds(row, R), :], turn, 1) for k in range(3)
                ]
                for k in range(2):
                    value = jnp.where(lanes < H - shift, turned[k], turned[k + 1])
                    value = jnp.where(live, value, 0.0)
                    patch[position, at, :, pl.ds(k * H, H)] = value
                    covered = covered + jnp.sum(value * value)
        cover[...] = covered

    take_patches(0)

    def half_planes(ref, mode):
        return read_plane(ref, 2 * mode), read_plane(ref, 2 * mode + 1)

    def run_batch(batch):
        for half in range(2):
            for chunk in range(CHUNKS):
                gbuf[half, 2 * CHUNKS + chunk, pl.ds(16, 8), :] = cover[...]

        @pl.loop(0, 2)
        def _(turn):
            half = (core + turn) % 2

            @pl.when(jnp.logical_and(turn == 1, batch > 0))
            def _():
                all_reduce_end(batch - 1)

            for mode in range(2):
                pr, pi = half_planes(pbuf.at[batch, half], mode)
                for position in range(POS):
                    our, oui = patch[position, 0], patch[position, 1]
                    psi = jnp.concatenate([pr * our - pi * oui, pr * oui + pi * our], axis=1)
                    left = left_product((table[0][...], table[1][...]), psi)
                    left = jnp.concatenate([left[:, :R], left[:, R:]], axis=0)
                    both = right_product(left, (table_t[0][...], table_t[1][...]))
                    quads = butterfly(both[:R], both[R:])
                    slot = half * 2 + mode
                    for a in range(2):
                        for b in range(2):
                            for at in range(2):
                                far[position, slot, at, pl.ds(a * HALF, HALF), pl.ds(b * HALF, HALF)] = (
                                    quads[a][b][at]
                                )

        for position in range(POS):
            for tile in range(R // 32):
                rows = pl.ds(tile * 32, 32)
                power = jnp.zeros((32, R), F32)
                for mode in range(MODES):
                    re, im = far[position, mode, 0, rows, :], far[position, mode, 1, rows, :]
                    power = power + re * re + im * im
                slot = batch * POS + position
                spat[slot, rows, :] = 1.0 - spat[slot, rows, :] * lax.rsqrt(power + 0.1)

        for turn in range(2):
            half = (core + 1 + turn) % 2
            for mode in range(2):
                pr, pi = half_planes(pbuf.at[batch, half], mode)
                sum_re, sum_im = None, None
                for position in range(POS):
                    slot = half * 2 + mode
                    quads = []
                    for a in range(2):
                        row = []
                        for b in range(2):
                            rows, cols = pl.ds(a * HALF, HALF), pl.ds(b * HALF, HALF)
                            keep = spat[batch * POS + position, rows, cols]
                            row.append(
                                (
                                    far[position, slot, 0, rows, cols] * keep,
                                    far[position, slot, 1, rows, cols] * keep,
                                )
                            )
                        quads.append(row)
                    both = butterfly_transposed(quads)
                    right = right_product(both, (table[0][...], table[1][...]))
                    right = jnp.concatenate([right[:R], right[R:]], axis=1)
                    back = left_product((table_t[0][...], table_t[1][...]), right)
                    dr, di = back[:, :R], back[:, R:]
                    our, oui = patch[position, 0], patch[position, 1]
                    og_re = pr * dr + pi * di
                    og_im = pr * di - pi * dr
                    if turn == 0 and mode == 0:
                        og[position, 0] = og_re
                        og[position, 1] = og_im
                    else:
                        og[position, 0] += og_re
                        og[position, 1] += og_im
                    pg_re = our * dr + oui * di
                    pg_im = our * di - oui * dr
                    sum_re = pg_re if sum_re is None else sum_re + pg_re
                    sum_im = pg_im if sum_im is None else sum_im + pg_im
                write_plane(gbuf.at[half], 2 * mode, sum_re)
                write_plane(gbuf.at[half], 2 * mode + 1, sum_im)
            if turn == 0:
                for part in range(PARTS):
                    to_sibling(batch, part).start()

    def add_gradient(batch):
        rows, firsts = [], []
        for position in range(POS):
            row, first, shift = window(batch * POS + position)
            rows.append(row)
            firsts.append(first)
            turn = shift % H
            for at in range(2):
                low = pltpu.roll(og[position, at, :, pl.ds(0, H)], turn, 1)
                high = pltpu.roll(og[position, at, :, pl.ds(H, H)], turn, 1)
                zbuf[position, at, 1, pl.ds(8, R), :] = jnp.where(lanes >= shift, low, 0.0)
                zbuf[position, at, 2, pl.ds(8, R), :] = jnp.where(lanes >= shift, high, low)
                zbuf[position, at, 3, pl.ds(8, R), :] = jnp.where(lanes >= shift, 0.0, high)

        def add_rows(base, which):
            for sub in range(2):
                at_row = pl.multiple_of(base + 8 * sub, 8)
                starts = [jnp.clip(at_row - row + 8, 0, R + 8) for row in rows]
                for at in range(2):
                    for lane in which:
                        value = grad[at, lane, pl.ds(at_row, 8), :]
                        for position in range(POS):
                            source = jnp.clip(lane - firsts[position] + 1, 0, 4)
                            value = value + zbuf[position, at, source, pl.ds(starts[position], 8), :]
                        grad[at, lane, pl.ds(at_row, 8), :] = value

        @pl.loop(0, 2 * H // 16)
        def _(tile):
            add_rows(tile * 16 + (tile // (H // 16)) * TILE, range(6))

        @pl.loop(0, TILE // 16)
        def _(tile):
            add_rows(H + tile * 16, (0, 5))

        border_turn(batch, 0)

        @pl.loop(0, TILE // 16)
        def _(tile):
            add_rows(H + tile * 16, range(1, 5))

    def border_copy(index):
        if index < 4:
            vertical, side = divmod(index, 2)
            rows = pl.ds(vertical * (H + TILE), H)
            return ways[side], True, neighbour_copy(
                grad.at[:, (0, 5)[side], rows, :], hcorn.at[vertical, side], gsend, grecv, index, ways[side]
            )
        if index < 12:
            piece, side = divmod(index - 4, 2)
            return ways[side], True, neighbour_copy(
                grad.at[:, (0, 5)[side], pl.ds(H + H * piece, H), :],
                hside.at[side, :, pl.ds(H * piece, H), :],
                gsend, grecv, index, ways[side],
            )
        lane = (1, 2, 0, 3)[(index - 12) // 2]
        vertical = (index - 12) % 2
        rows = pl.ds(vertical * (H + TILE), H)
        return ways[2 + vertical], True, neighbour_copy(
            grad.at[:, lane + 1, rows, :], hvert.at[vertical, :, lane], gsend, grecv, index, ways[2 + vertical]
        )

    def pass_corners():
        for index in range(4):
            vertical, side = divmod(index, 2)
            rows = pl.ds(vertical * (H + TILE), H)
            lane = (4, 1)[side]
            way, _, one = border_copy(index)

            @pl.when(there(back(way)))
            def _():
                one.wait_recv()
                for at in range(2):
                    grad[at, lane, rows, :] += hcorn[vertical, side, at]

    def border_turn(batch, turn):
        @pl.when(batch == BATCHES - 1)
        def _():
            if turn == 0:
                for index in range(4):
                    start_if(border_copy(index))
            if turn == 2:
                pass_corners()
            for index in (2 * turn + 12, 2 * turn + 13, 2 * turn + 4, 2 * turn + 5):
                start_if(border_copy(index))

    def to_sibling(batch, part):
        span = pl.ds(part * CHUNKS, CHUNKS)
        return pltpu.make_async_remote_copy(
            src_ref=gbuf.at[1 - core, span],
            dst_ref=recv0.at[batch, span],
            send_sem=bsend.at[part],
            recv_sem=brecv.at[batch, part],
            device_id=sibling,
            device_id_type=MESH,
        )

    def shared(batch, part, step):
        chunk = part * CHUNKS + 4 * ((place[ORDER[part][0]] + 4 - step) % 4)
        group = pl.ds(chunk, 4)
        index = part * 4 + step

        def copy(half):
            ref = pbuf.at[batch + 1, half, group, pl.ds(0, KEPT[part])]
            return pltpu.make_async_remote_copy(
                src_ref=ref,
                dst_ref=ref,
                send_sem=bsend.at[3 + index],
                recv_sem=brecv.at[batch, 3 + index],
                device_id=sibling,
                device_id_type=MESH,
            )

        return copy

    def all_reduce_end(batch):
        for step in range(4):
            for part in range(PARTS):
                shared(batch, part, step)(1 - core).wait_recv()
                shared(batch, part, step)(core).wait_send()

    def gather_sent(batch):
        for index in range(45):
            part = (index // 3) % 3
            ref = pbuf.at[batch + 1, core, part, pl.ds(0, KEPT[part])]
            pltpu.make_async_remote_copy(
                src_ref=ref,
                dst_ref=ref,
                send_sem=bsend.at[15 + 54 + index],
                recv_sem=brecv.at[batch, 0],
                device_id=sibling,
                device_id_type=MESH,
            ).wait_send()

    def all_reduce(batch):
        new = pbuf.at[batch + 1]
        old = pbuf.at[batch]

        def copy(source, target, index, to, send=0):
            return pltpu.make_async_remote_copy(
                src_ref=source,
                dst_ref=target,
                send_sem=bsend.at[send],
                recv_sem=brecv.at[batch, index],
                device_id=to,
                device_id_type=MESH,
            )

        sent = []

        def send(source, target, index, to):
            one = copy(source, target, index, to, 15 + len(sent))
            one.start()
            sent.append(one)

        def first_at(part, order):
            return (place[ORDER[part][1]] + 1 + order) % 4

        for part in range(PARTS):
            span = pl.ds(part * CHUNKS, CHUNKS)
            d1 = ORDER[part][0]
            to_sibling(batch, part).wait_recv()
            to_sibling(batch, part).wait_send()
            acc0[span] = gbuf[core, span] + recv0[batch, span]
            for order in range(4):
                for step in STEPS:
                    chunk = part * CHUNKS + 4 * ((place[d1] + step) % 4) + first_at(part, order)
                    target = recv1.at[batch, part, order, step - 1]
                    send(acc0.at[chunk], target, 15 + part * 4 + order, peer(d1, step))

        add_gradient(batch)

        @pl.when(batch > 0)
        def _():
            gather_sent(batch - 1)

        lasts = []
        for order in range(4):
            for part in range(PARTS):
                d1, d2, _ = ORDER[part]
                quarter = recv1.at[batch, part, order]
                copy(acc0.at[pl.ds(0, 3)], quarter, 15 + part * 4 + order, peer(d1, 1)).wait_recv()
                value = acc0[part * CHUNKS + 4 * place[d1] + first_at(part, order)]
                for step in STEPS:
                    value = value + quarter[step - 1]
                if order == 3:
                    lasts.append(value)
                else:
                    acc1[part, order] = value
                    target = recv2.at[batch, part, order]
                    send(acc1.at[part, order], target, 27 + part, peer(d2, order + 1))

        for part in range(PARTS):
            acc1[part, 3] = lasts[part]
        border_turn(batch, 1)

        @pl.when(batch < BATCHES - 1)
        def _():
            take_patches(batch + 1)

        for part in range(PARTS):
            _, d2, d3 = ORDER[part]
            copy(acc1.at[part, pl.ds(0, 3)], recv2.at[batch, part], 27 + part, peer(d2, 1)).wait_recv()
            value = acc1[part, 3]
            for step in STEPS:
                value = value + recv2[batch, part, step - 1]
            cross[batch, part, place[d3]] = value
            for step in STEPS:
                mine = cross.at[batch, part, place[d3]]
                send(mine, mine, 30 + part * 3 + step - 1, peer(d3, step))

        border_turn(batch, 2)
        for one in sent[:45]:
            one.wait_send()
        sums = []
        for part in range(PARTS):
            d3 = ORDER[part][2]
            for step in STEPS:
                theirs = cross.at[batch, part, (place[d3] + 4 - step) % 4]
                copy(theirs, theirs, 30 + part * 3 + step - 1, peer(d3, step)).wait_recv()
            value = cross[batch, part, 0]
            for at in range(1, 4):
                value = value + cross[batch, part, at]
            sums.append(value)
        scale = sums[2][16:] / float(R * R)
        scale = jnp.concatenate([scale, scale, scale], axis=0)

        def gather(part, chunk):
            d1 = ORDER[part][0]
            ref = new.at[core, chunk, pl.ds(0, KEPT[part])]
            for step in STEPS:
                send(ref, ref, 48 + part * 3 + step - 1, peer(d1, step))

        chunks = []
        for part in range(PARTS):
            d1, d2, _ = ORDER[part]
            chunk = part * CHUNKS + 4 * place[d1] + place[d2]
            chunks.append(chunk)
            new[core, chunk] = old[core, chunk] - sums[part] / scale
            for step in STEPS:
                mine = new.at[core, chunk, pl.ds(0, KEPT[part])]
                send(mine, mine, 39 + part * 3 + step - 1, peer(d2, step))
        for part in range(PARTS):
            gather(part, chunks[part])
        border_turn(batch, 3)
        for step in (1, 3, 2):
            for part in range(PARTS):
                d1, d2, _ = ORDER[part]
                chunk = part * CHUNKS + 4 * place[d1] + (place[d2] + 4 - step) % 4
                theirs = new.at[core, chunk, pl.ds(0, KEPT[part])]
                copy(theirs, theirs, 39 + part * 3 + step - 1, peer(d2, step)).wait_recv()
                gather(part, chunk)
        for part in range(PARTS):
            shared(batch, part, 0)(core).start()
        for step in (1, 3, 2):
            for part in range(PARTS):
                d1 = ORDER[part][0]
                group = new.at[
                    core, pl.ds(part * CHUNKS + 4 * ((place[d1] + 4 - step) % 4), 4), pl.ds(0, KEPT[part])
                ]
                copy(group, group, 48 + part * 3 + step - 1, peer(d1, step)).wait_recv()
                shared(batch, part, step)(core).start()
        for one in sent[45:54]:
            one.wait_send()

    @pl.loop(0, BATCHES)
    def _(batch):
        run_batch(batch)
        all_reduce(batch)

    power = jnp.zeros((R, R), F32)
    for turn in range(2):
        half = (core + turn) % 2
        if turn == 1:
            gather_sent(BATCHES - 1)
            all_reduce_end(BATCHES - 1)
        for plane in range(4):
            value = read_plane(pbuf.at[BATCHES, half], plane)
            probe_out[half * 2 + plane // 2, plane % 2] = value
            power = power + value * value
    part_of_top = 0.5 / jnp.max(power)

    for index in range(4, 20):
        wait_recv_if(border_copy(index))
    for index in range(20):
        wait_send_if(border_copy(index))

    def came(lane, row, rows, at):
        value = grad[at, lane + 1, pl.ds(H + row, rows), :]
        if lane == 0:
            value = value + hside[1, at, pl.ds(row, rows), :]
        if lane == 3:
            value = value + hside[0, at, pl.ds(row, rows), :]
        if row == 0:
            value = value + hvert[1, at, lane]
        if row == TILE - H:
            value = value + hvert[0, at, lane]
        return value

    for at in range(2):
        for lane in range(4):
            for row in range(0, TILE, H):
                place_at = (at, pl.ds(row, H), pl.ds(lane * H, H))
                obj_out[place_at] = obj[place_at] - came(lane, row, H, at) * part_of_top


def ship_kernel(obj, probe, obj_out, probe_out, sems):
    copies = [
        pltpu.make_async_copy(obj, obj_out, sems.at[0]),
        pltpu.make_async_copy(probe, probe_out, sems.at[1]),
    ]
    for one in copies:
        one.start()
    for one in copies:
        one.wait()


def local(object_field, probe, patterns, offsets, counts):
    vmem = pl.BlockSpec(memory_space=pltpu.VMEM)
    hbm = pl.BlockSpec(memory_space=pltpu.HBM)
    smem = pl.BlockSpec(memory_space=pltpu.SMEM)
    dma = pltpu.SemaphoreType.DMA
    done = pl.pallas_call(
        whole_kernel,
        out_shape=(
            pltpu.VMEM((2, TILE, TILE), F32),
            pltpu.VMEM((MODES, 2, R, R), F32),
        ),
        in_specs=[smem, smem, hbm, hbm, hbm, hbm],
        out_specs=(vmem, vmem),
        scratch_shapes=[
            pltpu.VMEM((2, TILE, TILE), F32),
            pltpu.VMEM((MODES, 2, R, R), F32),
            pltpu.VMEM((6, R, R), BF16),
            pltpu.VMEM((2, 6, TILE + 2 * H, H), F32),
            pltpu.VMEM((BATCHES + 1, 2, PARTS * CHUNKS, ROWS, R), F32),
            pltpu.VMEM((2, PARTS * CHUNKS, ROWS, R), F32),
            pltpu.VMEM((BATCHES * POS, R, R), F32),
            pltpu.VMEM((POS, 2, R, R), F32),
            pltpu.VMEM((POS, MODES, 2, R, R), F32),
            pltpu.VMEM((POS, 2, R, R), F32),
            pltpu.VMEM((POS, 2, 5, R + 16, H), F32),
            pltpu.VMEM((2, 6, TILE + 2 * H, H), F32),
            pltpu.VMEM((8, R), F32),
            pltpu.VMEM((PARTS * CHUNKS, ROWS, R), F32),
            pltpu.VMEM((PARTS, 4, ROWS, R), F32),
            pltpu.VMEM((BATCHES, PARTS * CHUNKS, ROWS, R), F32),
            pltpu.VMEM((BATCHES, PARTS, 4, 3, ROWS, R), F32),
            pltpu.VMEM((BATCHES, PARTS, 3, ROWS, R), F32),
            pltpu.VMEM((BATCHES, PARTS, 4, ROWS, R), F32),
            pltpu.VMEM((2, 2, TILE, H), F32),
            pltpu.VMEM((2, 2, 4, H, H), F32),
            pltpu.VMEM((2, 2, 2, H, H), F32),
            dma((4,)),
            dma((114,)),
            dma((BATCHES, 57)),
            dma((14,)),
            dma((14,)),
            dma((20,)),
            dma((20,)),
        ],
        compiler_params=pltpu.CompilerParams(
            collective_id=0, has_side_effects=True, vmem_limit_bytes=56 * 1024 * 1024
        ),
    )(
        offsets.reshape(BATCHES * POS, 2).T,
        counts.reshape(1),
        object_field,
        probe,
        patterns.reshape(BATCHES * POS, R, R),
        jnp.asarray(tables()),
    )
    return pl.pallas_call(
        ship_kernel,
        out_shape=(
            jax.ShapeDtypeStruct((2, TILE, TILE), F32),
            jax.ShapeDtypeStruct((MODES, 2, R, R), F32),
        ),
        in_specs=[vmem, vmem],
        out_specs=(hbm, hbm),
        scratch_shapes=[dma((2,))],
        compiler_params=pltpu.CompilerParams(vmem_limit_bytes=1024 * 1024),
    )(*done)


def solution(mesh):
    placed = (
        P(None, "narrow", "wide"),
        P(),
        P("narrow", "wide", None, None, None),
        P("narrow", "wide", None, None),
        P("narrow", "wide"),
    )
    return jax.shard_map(
        local,
        mesh=mesh,
        in_specs=placed,
        out_specs=(P(None, "narrow", "wide"), P()),
        check_vma=False,
    )
```
